512 devices in a mesh: grp: 32 (over z, x_hi, core), mem: 16 (over y, x_lo).
Axes of the slice: x: 4 (x_hi: 2, x_lo: 2; x = x_hi * 2 + x_lo), y: 8, z: 8, core: 2. Of those that a mesh axis runs over, the one named last changes fastest.
Arguments:
- hidden_grads: bfloat16 [65536, 2048], P(('grp', 'mem')), may hold values from -56 to 56
- weight_grad: bfloat16 [2048, 6144], P('mem', 'grp'), may hold values from -6 to 6
Outputs:
- inverse_root: float32 [2048, 2048], P('mem', 'grp')
- conditioned: float32 [2048, 6144], P('mem', 'grp')
The draws below stay inside these ranges and needn't reach their ends.
All inputs are finite; a program needn't handle non-finite values.
Results may differ from the reference program's by a relative error of at most 0.0003.
Values may be sent and summed in bfloat16 or wider, within the bound.
A program may use at most 64 MiB of HBM per device.

```python
import math
import jax
import jax.numpy as jnp
from jax import lax

D = 6144
BLK = 2048
ITERS = 2
TOKENS = 65536
N_GRP = 32
N_MEM = 16


def draw_hidden_grads(key, part):
    noise_key = jax.random.fold_in(key, 11)
    row_key = jax.random.fold_in(key, 12)
    col_key = jax.random.fold_in(key, 13)
    mixing_key = jax.random.fold_in(key, 14)
    token_pos = jnp.arange(TOKENS, dtype=jnp.float32) / TOKENS
    unit_pos = jnp.arange(BLK, dtype=jnp.float32) / BLK
    row_rough = jnp.exp(jax.random.uniform(row_key, (TOKENS,), jnp.float32, math.log(0.7), math.log(1.4)))
    col_rough = jnp.exp(jax.random.uniform(col_key, (BLK,), jnp.float32, math.log(0.7), math.log(1.4)))
    row_scale = jnp.power(10.0, 0.5 * token_pos) * row_rough
    col_scale = jnp.power(10.0, 0.25 * unit_pos) * col_rough
    noise = jnp.clip(jax.random.normal(noise_key, (TOKENS, BLK), jnp.float32), -5.0, 5.0)
    base = noise * row_scale[:, None] * col_scale[None, :]
    mixing = jax.random.normal(mixing_key, (BLK, BLK), jnp.float32) * (0.35 / math.sqrt(BLK))
    values = base + jnp.dot(base, mixing, precision=jax.lax.Precision.HIGHEST)
    values = jnp.clip(values, -56.0, 56.0)
    return values.astype(jnp.bfloat16)


def block_scale(key, shape, pieces, smallest, largest):
    loudness = 1.0
    for position, shards_of in pieces:
        steps = jax.random.uniform(jax.random.fold_in(jax.random.fold_in(key, 6), position), (shards_of,), jnp.float32, smallest / len(pieces), largest / len(pieces))
        loudness = loudness * jnp.repeat(jnp.exp(steps), shape[position] // shards_of).reshape((-1,) + (1,) * (len(shape) - 1 - position))
    return loudness


def centred(rng, extent, width, limit, shards=(), kind=jnp.bfloat16):
    entries = width * jax.random.normal(rng, extent, jnp.float32)
    if shards:
        entries = entries * block_scale(rng, extent, shards, -0.22, 0.18)
    return jnp.clip(entries, -limit, limit).astype(kind)


def setup_inputs(seed: int = 0) -> dict:
    arg_keys = jax.random.split(jax.random.key(seed), 3)
    return {
        "hidden_grads": draw_hidden_grads(jax.random.fold_in(arg_keys[2], 71), 0),
        "weight_grad": centred(arg_keys[1], (BLK, D), 1.0, 6.0, ((0, 16), (1, 32))),
    }


def reference(hidden_grads, weight_grad):
    exact_mode = lax.Precision.HIGHEST
    count = N_GRP * N_MEM
    blocks = hidden_grads.reshape(count, hidden_grads.shape[0] // count, hidden_grads.shape[1])

    def accumulate(running, block_rows):
        covariance, total_sq = running
        covariance = covariance + jnp.dot(block_rows.T, block_rows, preferred_element_type=jnp.float32)
        widened = block_rows.astype(jnp.float32)
        return (covariance, total_sq + jnp.sum(widened * widened)), None

    start_state = (jnp.zeros((BLK, BLK), jnp.float32), jnp.zeros((), jnp.float32))
    (covariance, total_sq), _ = lax.scan(accumulate, start_state, blocks)
    unit = jnp.eye(BLK, dtype=jnp.float32)
    iterate = covariance * (BLK / (6.0 * total_sq))
    root_mat = unit
    for step in range(ITERS):
        step_mat = 1.5 * unit - 0.5 * jnp.dot(root_mat, iterate, precision=exact_mode)
        iterate = jnp.dot(iterate, step_mat, precision=exact_mode)
        root_mat = jnp.dot(step_mat, root_mat, precision=exact_mode)
    conditioned = jnp.dot(root_mat, weight_grad.astype(jnp.float32), precision=exact_mode)
    return root_mat, conditioned
```

```python
import functools

import jax
import jax.numpy as jnp
from jax import lax
from jax.experimental import pallas as pl
from jax.experimental.pallas import tpu as pltpu
from jax.sharding import PartitionSpec as P

MESH = pl.DeviceIdType.MESH
F32 = jnp.float32
BF16 = jnp.bfloat16
CH = 4
ROWS = 128 // CH
rem = lax.rem
div = lax.div


def rcopy(src, dst, ssem, rsem, g, m):
    cp = pltpu.make_async_remote_copy(
        src_ref=src, dst_ref=dst, send_sem=ssem, recv_sem=rsem,
        device_id=(g, m), device_id_type=MESH,
    )
    cp.start()


def wait_bytes(ref, sem):
    pltpu.make_async_copy(ref, ref, sem).wait()


def wait_some(ref, sem, fewer):
    @pl.when(fewer)
    def _():
        wait_bytes(ref.at[pl.ds(0, ref.shape[0] - 1)], sem)

    @pl.when(jnp.logical_not(fewer))
    def _():
        wait_bytes(ref, sem)


def kernel(
    x_hbm, w_hbm, root_ref, cond_ref,
    xb, wv, sb, rb, ss, sso, ssx, ssb, yb, rowp, colp, exs, exr,
    ab, bb, rowp2, colp2, exs2, exr2, zb, zx, zp, wp, cxs, cxr,
    lsem, ag_send, ag_recv, fw_send, fw_recv, ss_sem, rs_send, rs_recv,
    sr_send, sr_recv, row_send, row_recv, col_send, col_recv, ex_send, ex_recv,
    w_send, w_recv,
):
    g = lax.axis_index("grp")
    m = lax.axis_index("mem")
    k, c = rem(g, 2), div(g, 2)
    z, xh = div(c, 2), rem(c, 2)
    y, xl = div(m, 2), rem(m, 2)
    x = 2 * xh + xl
    role = rem(x + 2 * y + z, 4)
    partner = c * 2 + 1 - k

    def place(xx, yy, zz, kk):
        return (zz * 2 + div(xx, 2)) * 2 + kk, yy * 2 + rem(xx, 2)

    own = 4 * k
    load_x = pltpu.make_async_copy(x_hbm, xb.at[pl.ds(own * 128, 128)], lsem.at[0])
    load_w = pltpu.make_async_copy(w_hbm, wv, lsem.at[1])
    load_x.start()
    load_w.start()

    def rows(slot, ch):
        return pl.ds(pl.multiple_of(slot * 128 + ch * ROWS, ROWS), ROWS)

    load_x.wait()
    near = (
        place(rem(x + 1 - k, 4), y, rem(z + k, 8), k),
        place(rem(x + 3 * (1 - k), 4), y, rem(z + 7 * k, 8), k),
        place(x, rem(y + 1 + 6 * k, 8), z, k),
    )
    for ch in range(CH):
        for j in range(3):
            rcopy(xb.at[rows(own, ch)], xb.at[rows(own + 1 + j, ch)],
                  ag_send, ag_recv.at[j, ch], *near[j])
    whole = pl.ds(pl.multiple_of(own * 128, 128), 128)
    rcopy(xb.at[whole], xb.at[whole], fw_send, fw_recv, partner, m)

    def squares(r):
        v = xb[r, :].astype(F32)
        s = jnp.sum(v * v, axis=0, keepdims=True)
        t = s[:, 0:128]
        for i in range(1, 16):
            t = t + s[:, i * 128:(i + 1) * 128]
        return t

    total = jnp.zeros((1, 128), F32)
    for ch in range(CH):
        total = total + squares(rows(own, ch))
    for ch in range(CH):
        for j in range(3):
            r = rows(own + 1 + j, ch)
            wait_bytes(xb.at[r], ag_recv.at[j, ch])
            rcopy(xb.at[r], xb.at[r], fw_send, fw_recv, partner, m)
            total = total + squares(r)
    ss[...] = total
    rcopy(ss, sso, ss_sem.at[0], ss_sem.at[1], partner, m)
    wait_bytes(xb.at[pl.ds(0, 512)], fw_recv)
    wait_bytes(sso, ss_sem.at[1])
    ssx[...] = ss[...] + sso[...]

    def cols(i):
        return xb[:, pl.ds(pl.multiple_of(i * 128, 128), 128)]

    @pl.loop(0, 4)
    def _(q):
        m0 = 8 * k + rem(role + 4 - q, 4)
        left = jnp.concatenate([cols(m0), cols(m0 + 4)], axis=1)
        zs = [rem(q, 2) + 2 * t for t in range(4)]
        cs = [2 * zt + rem(div(q + 8 - zt, 2), 2) for zt in zs]
        right = jnp.concatenate([cols(ct) for ct in cs], axis=1)
        part = lax.dot_general(left, right, (((0,), (0,)), ((), ())),
                               preferred_element_type=F32).astype(BF16)
        for a in range(2):
            yy = div(m0 + 4 * a, 2) - 4 * k
            for t in range(4):
                tile = part[a * 128:(a + 1) * 128, t * 128:(t + 1) * 128]
                sb[pl.ds((yy * 8 + zs[t]) * 2, 2)] = tile.reshape(2, 64, 128)

    slot = 8 * y + z

    @pl.loop(0, 32)
    def _(i):
        yo = rem(y + div(i, 8), 4)
        yy = 4 * k + yo
        zz = rem(z + rem(i, 8), 8)
        xx = rem(role + 24 - 2 * yy - zz, 4)
        for half in range(2):
            dg, dm = place(xx, yy, zz, half)
            piece = sb.at[(yo * 8 + zz) * 2 + half]
            mine = jnp.logical_and(dg == g, dm == m)

            @pl.when(mine)
            def _():
                rb[slot] = piece[...]
                ssb[slot] = ssx[...]

            @pl.when(jnp.logical_not(mine))
            def _():
                rcopy(piece, rb.at[slot], rs_send, rs_recv, dg, dm)
                rcopy(ssx, ssb.at[slot], sr_send, sr_recv, dg, dm)

    load_w.wait()
    at_home = div(y, 4) == k
    wait_some(rb, rs_recv, at_home)
    wait_some(ssb, sr_recv, at_home)

    def add8(i, acc):
        for j in range(8):
            acc = acc + rb[i * 8 + j].astype(F32)
        return acc

    cov = lax.fori_loop(0, 8, add8, jnp.zeros((64, 128), F32))
    total_sq = jnp.sum(ssb[...])
    scale = 2048.0 / (6.0 * total_sq)
    it = cov * scale
    row_core, col_core = div(c, 8), div(m, 8)
    row_slot = 2 * rem(c, 8) + k
    col_slot = 2 * rem(m, 8) + k
    own_row, own_col = row_core == k, col_core == k

    def along_row(src, dst, n):
        @pl.loop(0, 16)
        def _(i):
            dg = 2 * rem(c + i, 16) + row_core

            @pl.when(dg == g)
            def _():
                dst[row_slot] = src[...]

            @pl.when(dg != g)
            def _():
                rcopy(src, dst.at[row_slot], row_send.at[n], row_recv.at[n], dg, m)

    def along_col(src, dst, n):
        @pl.loop(0, 16)
        def _(i):
            dg, dm = 2 * c + col_core, rem(m + i, 16)
            mine = jnp.logical_and(dg == g, dm == m)

            @pl.when(mine)
            def _():
                dst[col_slot] = src[...]

            @pl.when(jnp.logical_not(mine))
            def _():
                rcopy(src, dst.at[col_slot], col_send.at[n], col_recv.at[n], dg, dm)

    def spread_w():
        @pl.loop(0, 16)
        def _(i):
            dg, dm = 2 * c + col_core, rem(m + i, 16)
            mine = jnp.logical_and(dg == g, dm == m)

            @pl.when(mine)
            def _():
                wp[col_slot] = wv[...]

            @pl.when(jnp.logical_not(mine))
            def _():
                rcopy(wv, wp.at[col_slot], w_send, w_recv, dg, dm)

    def side_by_side(ref):
        return jnp.concatenate(
            [ref[2 * j:2 * j + 2].reshape(128, 128) for j in range(8)], axis=1)

    def tile_product(lp, rp, out, got, n):
        out[...] = jnp.dot(side_by_side(lp), rp[...].reshape(1024, 128),
                           preferred_element_type=F32)
        other = pl.ds(pl.multiple_of(64 * (1 - k), 64), 64)
        rcopy(out.at[other], got, ex_send.at[n], ex_recv.at[n], partner, m)
        mine = out[pl.ds(pl.multiple_of(64 * k, 64), 64), :]
        wait_bytes(got, ex_recv.at[n])
        return mine + got[...]

    yb[...] = it.astype(BF16)
    along_row(yb, rowp, 0)
    along_col(yb, colp, 0)
    spread_w()
    wait_some(rowp, row_recv.at[0], own_row)
    wait_some(colp, col_recv.at[0], own_col)
    sq = tile_product(rowp, colp, exs, exr, 0)

    ab[...] = sq.astype(BF16)
    bb[...] = (0.0625 * sq - 0.5625 * it).astype(BF16)
    along_row(ab, rowp2, 1)
    along_col(bb, colp2, 1)
    wait_some(rowp2, row_recv.at[1], own_row)
    wait_some(colp2, col_recv.at[1], own_col)
    higher = tile_product(rowp2, colp2, exs2, exr2, 1)

    row_ids = m * 128 + 64 * k + lax.broadcasted_iota(jnp.int32, (64, 128), 0)
    col_ids = c * 128 + lax.broadcasted_iota(jnp.int32, (64, 128), 1)
    unit = jnp.where(row_ids == col_ids, 2.25, 0.0).astype(F32)
    zz_tile = unit - 2.4375 * it + 1.6875 * sq + higher
    zb[...] = zz_tile
    along_row(zb, zp, 2)
    rcopy(zb, zx, ex_send.at[2], ex_recv.at[2], partner, m)

    def half_lanes(v):
        return jnp.where(k == 0, v[:, :64], v[:, 64:])

    root_ref[pl.ds(pl.multiple_of(64 * k, 64), 64), :] = half_lanes(zz_tile)
    wait_bytes(zx, ex_recv.at[2])
    root_ref[pl.ds(pl.multiple_of(64 * (1 - k), 64), 64), :] = half_lanes(zx[...])

    wait_some(wp, w_recv, own_col)
    wait_some(zp, row_recv.at[2], own_row)
    left = side_by_side(zp)
    hi = left.astype(BF16)
    lo = (left - hi.astype(F32)).astype(BF16)

    def weighted(kk):
        right = jnp.concatenate([wp[2 * j + kk] for j in range(8)], axis=0)
        return (jnp.dot(hi, right, preferred_element_type=F32)
                + jnp.dot(lo, right, preferred_element_type=F32))

    cxs[...] = weighted(1 - k)
    rcopy(cxs, cxr, ex_send.at[3], ex_recv.at[3], partner, m)
    out = weighted(k)
    wait_bytes(cxr, ex_recv.at[3])
    cond_ref[...] = out + cxr[...]

    wait_bytes(xb.at[pl.ds(0, 384)], ag_send)
    wait_bytes(xb.at[pl.ds(0, 512)], fw_send)
    wait_bytes(ss, ss_sem.at[0])
    wait_some(sb, rs_send, at_home)
    wait_some(ssb, sr_send, at_home)
    wait_some(rowp, row_send.at[0], own_row)
    wait_some(colp, col_send.at[0], own_col)
    wait_some(rowp2, row_send.at[1], own_row)
    wait_some(colp2, col_send.at[1], own_col)
    wait_some(zp, row_send.at[2], own_row)
    wait_some(wp, w_send, own_col)
    wait_bytes(exr, ex_send.at[0])
    wait_bytes(exr2, ex_send.at[1])
    wait_bytes(zx, ex_send.at[2])
    wait_bytes(cxr, ex_send.at[3])


def on_device(hidden_grads, weight_grad):
    dma = pltpu.SemaphoreType.DMA
    vm = pltpu.VMEM
    return pl.pallas_call(
        kernel,
        out_shape=(jax.ShapeDtypeStruct((128, 64), F32), jax.ShapeDtypeStruct((128, 192), F32)),
        in_specs=[pl.BlockSpec(memory_space=pl.ANY)] * 2,
        out_specs=(pl.BlockSpec(memory_space=pltpu.VMEM),) * 2,
        scratch_shapes=[
            vm((1024, 2048), BF16),
            vm((128, 192), BF16),
            vm((64, 64, 128), BF16),
            vm((64, 64, 128), BF16),
            vm((1, 128), F32), vm((1, 128), F32), vm((1, 128), F32),
            vm((64, 1, 128), F32),
            vm((64, 128), BF16),
            vm((16, 64, 128), BF16), vm((16, 64, 128), BF16),
            vm((128, 128), F32), vm((64, 128), F32),
            vm((64, 128), BF16), vm((64, 128), BF16),
            vm((16, 64, 128), BF16), vm((16, 64, 128), BF16),
            vm((128, 128), F32), vm((64, 128), F32),
            vm((64, 128), F32), vm((64, 128), F32),
            vm((16, 64, 128), F32),
            vm((16, 128, 192), BF16),
            vm((128, 192), F32), vm((128, 192), F32),
            dma((2,)), dma, dma((3, CH)), dma, dma, dma((2,)), dma, dma,
            dma, dma, dma((3,)), dma((3,)), dma((2,)), dma((2,)), dma((4,)), dma((4,)),
            dma, dma,
        ],
        compiler_params=pltpu.CompilerParams(has_side_effects=True, vmem_limit_bytes=48 * 1024 * 1024),
        name="kfac",
    )(hidden_grads, weight_grad)


def solution(mesh):
    spec = P("mem", "grp")
    return jax.shard_map(
        on_device,
        mesh=mesh,
        in_specs=(P(("grp", "mem"), None), spec),
        out_specs=(spec, spec),
        check_vma=False,
    )
```

```python
import functools

import jax
import jax.numpy as jnp
from jax import lax
from jax.experimental import pallas as pl
from jax.experimental.pallas import tpu as pltpu
from jax.sharding import PartitionSpec as P

MESH = pl.DeviceIdType.MESH
F32 = jnp.float32
BF16 = jnp.bfloat16
CH = 4
ROWS = 128 // CH
rem = lax.rem
div = lax.div


def rcopy(src, dst, ssem, rsem, g, m):
    cp = pltpu.make_async_remote_copy(
        src_ref=src, dst_ref=dst, send_sem=ssem, recv_sem=rsem,
        device_id=(g, m), device_id_type=MESH,
    )
    cp.start()


def wait_bytes(ref, sem):
    pltpu.make_async_copy(ref, ref, sem).wait()


def wait_some(ref, sem, fewer):
    @pl.when(fewer)
    def _():
        wait_bytes(ref.at[pl.ds(0, ref.shape[0] - 1)], sem)

    @pl.when(jnp.logical_not(fewer))
    def _():
        wait_bytes(ref, sem)


def kernel(
    x_hbm, w_hbm, root_ref, cond_ref,
    xb, wv, sb, ra, sb2, rb, ss, sso, ssx, ssa, ssy, ssb, yb, rowp, colp, exs, exr,
    ab, bb, rowp2, colp2, exs2, exr2, zb, zx, qb, qp, wp, cxs, cxr,
    lsem, ag_send, ag_recv, fw_send, fw_recv, ss_sem, rs_send, rs_recv, rs2_send, rs2_recv,
    sr_send, sr_recv, row_send, row_recv, col_send, col_recv, ex_send, ex_recv,
    w_send, w_recv,
):
    g = lax.axis_index("grp")
    m = lax.axis_index("mem")
    k, c = rem(g, 2), div(g, 2)
    z, xh = div(c, 2), rem(c, 2)
    y, xl = div(m, 2), rem(m, 2)
    x = 2 * xh + xl
    role = rem(x + 2 * y + z, 4)
    partner = c * 2 + 1 - k

    def place(xx, yy, zz, kk):
        return (zz * 2 + div(xx, 2)) * 2 + kk, yy * 2 + rem(xx, 2)

    own = 4 * k
    load_x = pltpu.make_async_copy(x_hbm, xb.at[pl.ds(own * 128, 128)], lsem.at[0])
    load_w = pltpu.make_async_copy(w_hbm, wv, lsem.at[1])
    load_x.start()
    load_w.start()

    barrier = pltpu.get_barrier_semaphore()

    def greet(dg, dm):
        pl.semaphore_signal(barrier, inc=1, device_id=(dg, dm), device_id_type=MESH)

    def diagonal(dy, dz):
        yy, zz = rem(y + dy, 8), rem(z + dz, 8)
        return rem(role + 24 - 2 * yy - zz, 4), yy, zz

    greet(partner, m)
    for step in (1, 7):
        greet(*place(rem(x + step * (1 - k), 4), y, rem(z + step * k, 8), k))
        greet(*place(x, rem(y + step, 8), z, k))

    @pl.loop(1, 8)
    def _(i):
        for half in range(2):
            greet(*place(*diagonal(i, 0), half))
            greet(*place(*diagonal(0, i), half))

    @pl.loop(1, 16)
    def _(i):
        for half in range(2):
            greet(2 * rem(c + i, 16) + half, m)
            greet(2 * c + half, rem(m + i, 16))

    pl.semaphore_wait(barrier, 5 + 28 + 60)

    def rows(slot, ch):
        return pl.ds(pl.multiple_of(slot * 128 + ch * ROWS, ROWS), ROWS)

    pending = []

    load_x.wait()
    near = (
        place(rem(x + 1 - k, 4), y, rem(z + k, 8), k),
        place(rem(x + 3 * (1 - k), 4), y, rem(z + 7 * k, 8), k),
        place(x, rem(y + 1 + 6 * k, 8), z, k),
    )
    for ch in range(CH):
        for j in range(3):
            rcopy(xb.at[rows(own, ch)], xb.at[rows(own + 1 + j, ch)],
                  ag_send, ag_recv.at[j, ch], *near[j])
    whole = pl.ds(pl.multiple_of(own * 128, 128), 128)
    rcopy(xb.at[whole], xb.at[whole], fw_send, fw_recv, partner, m)
    pending.append(lambda: wait_bytes(xb.at[pl.ds(0, 384)], ag_send))
    pending.append(lambda: wait_bytes(xb.at[pl.ds(0, 512)], fw_send))

    load_w.wait()
    w_slot = 8 * xl + 2 * rem(y, 4) + k
    w_core = div(y, 4)
    w_kept = w_core == k

    @pl.loop(1, 9)
    def _(i):
        mine = jnp.logical_and(i == 8, w_kept)

        @pl.when(mine)
        def _():
            wp[w_slot] = wv[...]

        @pl.when(jnp.logical_not(mine))
        def _():
            rcopy(wv, wp.at[w_slot], w_send.at[0], w_recv.at[0], *place(x, rem(y + i, 8), z, w_core))

    w_mine = pl.ds(8 * xl, 8)
    pending.append(lambda: wait_some(wp.at[pl.ds(0, 8)], w_send.at[0], w_kept))

    def squares(r):
        v = xb[r, :].astype(F32)
        s = jnp.sum(v * v, axis=0, keepdims=True)
        t = s[:, 0:128]
        for i in range(1, 16):
            t = t + s[:, i * 128:(i + 1) * 128]
        return t

    total = jnp.zeros((1, 128), F32)
    for ch in range(CH):
        total = total + squares(rows(own, ch))
    for ch in range(CH):
        for j in range(3):
            r = rows(own + 1 + j, ch)
            wait_bytes(xb.at[r], ag_recv.at[j, ch])
            rcopy(xb.at[r], xb.at[r], fw_send, fw_recv, partner, m)
            total = total + squares(r)
    ss[...] = total
    rcopy(ss, sso, ss_sem.at[0], ss_sem.at[1], partner, m)
    pending.append(lambda: wait_bytes(ss, ss_sem.at[0]))
    wait_bytes(xb.at[pl.ds(0, 512)], fw_recv)
    wait_bytes(sso, ss_sem.at[1])
    ssx[...] = ss[...] + sso[...]

    def cols(i):
        return xb[:, pl.ds(pl.multiple_of(i * 128, 128), 128)]

    @pl.loop(0, 4)
    def _(q):
        m0 = 8 * k + rem(role + 4 - q, 4)
        left = jnp.concatenate([cols(m0), cols(m0 + 4)], axis=1)
        zs = [rem(q, 2) + 2 * t for t in range(4)]
        cs = [2 * zt + rem(div(q + 8 - zt, 2), 2) for zt in zs]
        right = jnp.concatenate([cols(ct) for ct in cs], axis=1)
        part = lax.dot_general(left, right, (((0,), (0,)), ((), ())),
                               preferred_element_type=F32).astype(BF16)
        for a in range(2):
            yo = div(m0 + 4 * a, 2) - 4 * k
            for t in range(4):
                tile = part[a * 128:(a + 1) * 128, t * 128:(t + 1) * 128]
                sb[0, zs[t] * 4 + yo] = tile[:64]
                sb[1, yo * 8 + zs[t]] = tile[64:]

    first_slot = z * (1 - k) + y * k
    second_slot = y * (1 - k) + z * k
    in_half = div(y, 4) == k
    on_low = k == 0

    @pl.loop(1, 9)
    def _(i):
        xx, yy, zz = diagonal(0, i)
        dg, dm = place(xx, yy, zz, 0)
        piece = sb.at[0, pl.ds(zz * 4, 4)]
        there = pl.ds(z * 8 + 4 * k, 4)
        mine = jnp.logical_and(on_low, i == 8)

        @pl.when(mine)
        def _():
            ra[there] = piece[...]

        @pl.when(jnp.logical_not(mine))
        def _():
            rcopy(piece, ra.at[there], rs_send.at[0], rs_recv, dg, dm)

    @pl.loop(1, 5)
    def _(i):
        yo = rem(y + i, 4)
        yy = 4 * k + yo
        xx = rem(role + 24 - 2 * yy - z, 4)
        dg, dm = place(xx, yy, z, 1)
        piece = sb.at[1, pl.ds(yo * 8, 8)]
        there = pl.ds(y * 8, 8)
        mine = jnp.logical_and(k == 1, yy == y)

        @pl.when(mine)
        def _():
            ra[there] = piece[...]

        @pl.when(jnp.logical_not(mine))
        def _():
            rcopy(piece, ra.at[there], rs_send.at[1], rs_recv, dg, dm)

    wait_some(wp.at[pl.ds(0, 8)], w_recv.at[0], w_kept)
    rcopy(wp.at[w_mine], wp.at[w_mine], w_send.at[1], w_recv.at[1], *place(2 * xh + 1 - xl, y, z, k))
    pending.append(lambda: wait_bytes(wp.at[pl.ds(0, 8)], w_send.at[1]))
    ssa[first_slot] = ssx[...]

    @pl.loop(1, 8)
    def _(i):
        dg, dm = place(*diagonal(k * i, (1 - k) * i), k)
        rcopy(ssx, ssa.at[first_slot], sr_send.at[0], sr_recv.at[0], dg, dm)

    def wait_first(sem, sending):
        full = sb.at[0]
        if sending:
            pl.when(on_low)(lambda: wait_bytes(full.at[pl.ds(0, 28)], sem.at[0]))
            pl.when(k == 1)(lambda: wait_bytes(full, sem.at[0]))
            kept = jnp.logical_and(k == 1, in_half)
            pl.when(kept)(lambda: wait_bytes(full.at[pl.ds(0, 24)], sem.at[1]))
            pl.when(jnp.logical_not(kept))(lambda: wait_bytes(full, sem.at[1]))
        else:
            kept = jnp.logical_and(k == 1, in_half)
            pl.when(on_low)(lambda: wait_bytes(ra.at[pl.ds(0, 60)], sem))
            pl.when(kept)(lambda: wait_bytes(ra.at[pl.ds(0, 56)], sem))
            pl.when(jnp.logical_and(k == 1, jnp.logical_not(in_half)))(lambda: wait_bytes(ra, sem))

    pending.append(lambda: wait_first(rs_send, True))
    pending.append(lambda: wait_bytes(ssa.at[pl.ds(0, 7)], sr_send.at[0]))
    wait_first(rs_recv, False)
    wait_bytes(ssa.at[pl.ds(0, 7)], sr_recv.at[0])
    ssy[...] = jnp.sum(ssa[...], axis=0)

    @pl.loop(1, 9)
    def _(i):
        to = rem(second_slot + i, 8)
        acc = ra[to].astype(F32)
        for j in range(1, 8):
            acc = acc + ra[j * 8 + to].astype(F32)
        dg, dm = place(*diagonal((1 - k) * i, k * i), k)

        @pl.when(i == 8)
        def _():
            rb[second_slot] = acc
            ssb[second_slot] = ssy[...]

        @pl.when(i < 8)
        def _():
            sb2[to] = acc
            rcopy(sb2.at[to], rb.at[second_slot], rs2_send, rs2_recv, dg, dm)
            rcopy(ssy, ssb.at[second_slot], sr_send.at[1], sr_recv.at[1], dg, dm)

    pending.append(lambda: wait_bytes(rb.at[pl.ds(0, 7)], rs2_send))
    pending.append(lambda: wait_bytes(ssb.at[pl.ds(0, 7)], sr_send.at[1]))
    wait_bytes(rb.at[pl.ds(0, 7)], rs2_recv)
    wait_bytes(ssb.at[pl.ds(0, 7)], sr_recv.at[1])
    cov = rb[0]
    for j in range(1, 8):
        cov = cov + rb[j]
    total_sq = jnp.sum(ssb[...])
    scale = 2048.0 / (6.0 * total_sq)
    it = cov * scale
    row_core, col_core = div(c, 8), div(m, 8)
    row_slot = 2 * rem(c, 8) + k
    col_slot = 2 * rem(m, 8) + k
    own_row, own_col = row_core == k, col_core == k

    def along_row(src, dst, n):
        @pl.loop(0, 16)
        def _(i):
            dg = 2 * rem(c + i, 16) + row_core

            @pl.when(dg == g)
            def _():
                dst[row_slot] = src[...]

            @pl.when(dg != g)
            def _():
                rcopy(src, dst.at[row_slot], row_send.at[n], row_recv.at[n], dg, m)

    def along_col(src, dst, n):
        @pl.loop(0, 16)
        def _(i):
            dg, dm = 2 * c + col_core, rem(m + i, 16)
            mine = jnp.logical_and(dg == g, dm == m)

            @pl.when(mine)
            def _():
                dst[col_slot] = src[...]

            @pl.when(jnp.logical_not(mine))
            def _():
                rcopy(src, dst.at[col_slot], col_send.at[n], col_recv.at[n], dg, dm)

    def side_by_side(ref):
        return jnp.concatenate(
            [ref[2 * j:2 * j + 2].reshape(128, 128) for j in range(8)], axis=1)

    def tile_product(lp, rp, out, got, n):
        out[...] = jnp.dot(side_by_side(lp), rp[...].reshape(1024, 128),
                           preferred_element_type=F32)
        other = pl.ds(pl.multiple_of(64 * (1 - k), 64), 64)
        rcopy(out.at[other], got, ex_send.at[n], ex_recv.at[n], partner, m)
        mine = out[pl.ds(pl.multiple_of(64 * k, 64), 64), :]
        wait_bytes(got, ex_recv.at[n])
        return mine + got[...]

    it16 = it.astype(BF16)
    yb[...] = it16
    along_row(yb, rowp, 0)
    along_col(yb, colp, 0)
    pending.append(lambda: wait_some(rowp, row_send.at[0], own_row))
    pending.append(lambda: wait_some(colp, col_send.at[0], own_col))
    wait_some(rowp, row_recv.at[0], own_row)
    wait_some(colp, col_recv.at[0], own_col)
    sq = tile_product(rowp, colp, exs, exr, 0)
    pending.append(lambda: wait_bytes(exr, ex_send.at[0]))

    sq16 = sq.astype(BF16)
    ab[...] = sq16
    bb[...] = (0.0625 * sq - 0.5625 * it).astype(BF16)
    along_row(ab, rowp2, 1)
    along_col(bb, colp2, 1)
    pending.append(lambda: wait_some(rowp2, row_send.at[1], own_row))
    pending.append(lambda: wait_some(colp2, col_send.at[1], own_col))
    wait_some(rowp2, row_recv.at[1], own_row)
    wait_some(colp2, col_recv.at[1], own_col)
    higher = tile_product(rowp2, colp2, exs2, exr2, 1)
    pending.append(lambda: wait_bytes(exr2, ex_send.at[1]))

    row_ids = m * 128 + 64 * k + lax.broadcasted_iota(jnp.int32, (64, 128), 0)
    col_ids = c * 128 + lax.broadcasted_iota(jnp.int32, (64, 128), 1)
    unit = jnp.where(row_ids == col_ids, 2.25, 0.0).astype(F32)
    zz_tile = unit - 2.4375 * it + 1.6875 * sq + higher
    qb[...] = (higher - 2.4375 * (it - it16.astype(F32)) + 1.6875 * (sq - sq16.astype(F32))).astype(BF16)
    along_row(qb, qp, 2)
    zb[...] = zz_tile
    rcopy(zb, zx, ex_send.at[2], ex_recv.at[2], partner, m)
    pending.append(lambda: wait_some(qp, row_send.at[2], own_row))
    pending.append(lambda: wait_bytes(zx, ex_send.at[2]))

    def half_lanes(v):
        return jnp.where(k == 0, v[:, :64], v[:, 64:])

    root_ref[pl.ds(pl.multiple_of(64 * k, 64), 64), :] = half_lanes(zz_tile)
    wait_bytes(zx, ex_recv.at[2])
    root_ref[pl.ds(pl.multiple_of(64 * (1 - k), 64), 64), :] = half_lanes(zx[...])

    wait_bytes(wp.at[pl.ds(0, 8)], w_recv.at[1])
    left = 1.6875 * side_by_side(rowp2).astype(F32) - 2.4375 * side_by_side(rowp).astype(F32)
    hi = left.astype(BF16)
    lo = (left - hi.astype(F32)).astype(BF16)

    def right(kk):
        return jnp.concatenate([wp[8 * (j % 2) + 2 * (j // 2) + kk] for j in range(8)], axis=0)

    def known(kk):
        return (jnp.dot(hi, right(kk), preferred_element_type=F32)
                + jnp.dot(lo, right(kk), preferred_element_type=F32))

    cxs[...] = known(1 - k)
    cond_ref[...] = known(k) + 2.25 * wv[...].astype(F32)
    wait_some(qp, row_recv.at[2], own_row)
    rest = side_by_side(qp)
    cxs[...] += jnp.dot(rest, right(1 - k), preferred_element_type=F32)
    rcopy(cxs, cxr, ex_send.at[3], ex_recv.at[3], partner, m)
    pending.append(lambda: wait_bytes(cxr, ex_send.at[3]))
    cond_ref[...] += jnp.dot(rest, right(k), preferred_element_type=F32)
    wait_bytes(cxr, ex_recv.at[3])
    cond_ref[...] += cxr[...]

    for finish in pending:
        finish()


def on_device(hidden_grads, weight_grad):
    dma = pltpu.SemaphoreType.DMA
    vm = pltpu.VMEM
    return pl.pallas_call(
        kernel,
        out_shape=(jax.ShapeDtypeStruct((128, 64), F32), jax.ShapeDtypeStruct((128, 192), F32)),
        in_specs=[pl.BlockSpec(memory_space=pl.ANY)] * 2,
        out_specs=(pl.BlockSpec(memory_space=pltpu.VMEM),) * 2,
        scratch_shapes=[
            vm((1024, 2048), BF16),
            vm((128, 192), BF16),
            vm((2, 32, 64, 128), BF16),
            vm((64, 64, 128), BF16),
            vm((8, 64, 128), F32), vm((8, 64, 128), F32),
            vm((1, 128), F32), vm((1, 128), F32), vm((1, 128), F32),
            vm((8, 1, 128), F32), vm((1, 128), F32), vm((8, 1, 128), F32),
            vm((64, 128), BF16),
            vm((16, 64, 128), BF16), vm((16, 64, 128), BF16),
            vm((128, 128), F32), vm((64, 128), F32),
            vm((64, 128), BF16), vm((64, 128), BF16),
            vm((16, 64, 128), BF16), vm((16, 64, 128), BF16),
            vm((128, 128), F32), vm((64, 128), F32),
            vm((64, 128), F32), vm((64, 128), F32),
            vm((64, 128), BF16), vm((16, 64, 128), BF16),
            vm((16, 128, 192), BF16),
            vm((128, 192), F32), vm((128, 192), F32),
            dma((2,)), dma, dma((3, CH)), dma, dma, dma((2,)), dma((2,)), dma,
            dma, dma, dma((2,)), dma((2,)), dma((3,)), dma((3,)), dma((2,)), dma((2,)), dma((4,)), dma((4,)),
            dma((2,)), dma((2,)),
        ],
        compiler_params=pltpu.CompilerParams(has_side_effects=True, collective_id=0, vmem_limit_bytes=48 * 1024 * 1024),
        name="kfac",
    )(hidden_grads, weight_grad)


def solution(mesh):
    spec = P("mem", "grp")
    return jax.shard_map(
        on_device,
        mesh=mesh,
        in_specs=(P(("grp", "mem"), None), spec),
        out_specs=(spec, spec),
        check_vma=False,
    )
```

```python
import functools

import jax
import jax.numpy as jnp
from jax import lax
from jax.experimental import pallas as pl
from jax.experimental.pallas import tpu as pltpu
from jax.sharding import PartitionSpec as P

MESH = pl.DeviceIdType.MESH
F32 = jnp.float32
BF16 = jnp.bfloat16
CH = 4
ROWS = 128 // CH
rem = lax.rem
div = lax.div


def rcopy(src, dst, ssem, rsem, g, m):
    cp = pltpu.make_async_remote_copy(
        src_ref=src, dst_ref=dst, send_sem=ssem, recv_sem=rsem,
        device_id=(g, m), device_id_type=MESH,
    )
    cp.start()


def wait_bytes(ref, sem):
    pltpu.make_async_copy(ref, ref, sem).wait()


def wait_some(ref, sem, fewer):
    @pl.when(fewer)
    def _():
        wait_bytes(ref.at[pl.ds(0, ref.shape[0] - 1)], sem)

    @pl.when(jnp.logical_not(fewer))
    def _():
        wait_bytes(ref, sem)


def kernel(
    x_hbm, w_hbm, root_ref, cond_ref,
    xb, wv, sb, ra, sb2, rb, ss, sso, ssx, ssa, ssy, ssb, yb, rowp, colp, exs, exr,
    ab, bb, rowp2, colp2, exs2, exr2, zb, zx, whole_tile, qb, qp, wp, cxs, cxr,
    lsem, ag_send, ag_recv, fw_send, fw_recv, ss_sem, rs_send, rs_recv, rs2_send, rs2_recv,
    sr_send, sr_recv, row_send, row_recv, col_send, col_recv, ex_send, ex_recv,
    w_send, w_recv, met,
):
    g = lax.axis_index("grp")
    m = lax.axis_index("mem")
    k, c = rem(g, 2), div(g, 2)
    z, xh = div(c, 2), rem(c, 2)
    y, xl = div(m, 2), rem(m, 2)
    x = 2 * xh + xl
    role = rem(x + 2 * y + z, 4)
    partner = c * 2 + 1 - k

    def place(xx, yy, zz, kk):
        return (zz * 2 + div(xx, 2)) * 2 + kk, yy * 2 + rem(xx, 2)

    own = 4 * k
    load_x = pltpu.make_async_copy(x_hbm, xb.at[pl.ds(own * 128, 128)], lsem.at[0])
    load_w = pltpu.make_async_copy(w_hbm, wv, lsem.at[1])
    load_x.start()
    load_w.start()

    barrier = pltpu.get_barrier_semaphore()

    def greet(dg, dm):
        pl.semaphore_signal(barrier, inc=1, device_id=(dg, dm), device_id_type=MESH)

    def diagonal(dy, dz):
        yy, zz = rem(y + dy, 8), rem(z + dz, 8)
        return rem(role + 24 - 2 * yy - zz, 4), yy, zz

    greet(partner, m)
    for step in (1, 7):
        greet(*place(rem(x + step, 4), y, z, k))
        greet(*place(x, rem(y + step, 8), z, k))
        greet(*place(x, y, rem(z + step, 8), k))
    pl.semaphore_wait(barrier, 7)

    def introduce():
        def nudge(n, dg, dm):
            pl.semaphore_signal(met.at[n], inc=1, device_id=(dg, dm), device_id_type=MESH)

        for step in (1, 3):
            nudge(0, *place(rem(x + step, 4), y, z, k))
        pl.semaphore_wait(met.at[0], 2)
        for n, steps in ((1, (1, 7)), (2, (2, 6))):
            for step in steps:
                nudge(n, *place(x, rem(y + step, 8), z, k))
                nudge(n, *place(x, y, rem(z + step, 8), k))
            pl.semaphore_wait(met.at[n], 4)
        nudge(3, partner, m)
        pl.semaphore_wait(met.at[3], 1)

    def rows(slot, ch):
        return pl.ds(pl.multiple_of(slot * 128 + ch * ROWS, ROWS), ROWS)

    def diagonal(dy, dz):
        yy, zz = rem(y + dy, 8), rem(z + dz, 8)
        return rem(role + 24 - 2 * yy - zz, 4), yy, zz

    pending = []

    load_x.wait()
    near = (
        place(rem(x + 1 - k, 4), y, rem(z + k, 8), k),
        place(rem(x + 3 * (1 - k), 4), y, rem(z + 7 * k, 8), k),
        place(x, rem(y + 1 + 6 * k, 8), z, k),
    )
    for ch in range(CH):
        for j in range(3):
            rcopy(xb.at[rows(own, ch)], xb.at[rows(own + 1 + j, ch)],
                  ag_send, ag_recv.at[j, ch], *near[j])
    whole = pl.ds(pl.multiple_of(own * 128, 128), 128)
    rcopy(xb.at[whole], xb.at[whole], fw_send, fw_recv, partner, m)
    pending.append(lambda: wait_bytes(xb.at[pl.ds(0, 384)], ag_send))
    pending.append(lambda: wait_bytes(xb.at[pl.ds(0, 512)], fw_send))

    load_w.wait()
    w_slot = 8 * xl + 2 * rem(y, 4) + k
    w_core = div(y, 4)
    w_kept = w_core == k

    def spread_w():
        @pl.loop(1, 9)
        def _(i):
            mine = jnp.logical_and(i == 8, w_kept)

            @pl.when(mine)
            def _():
                wp[w_slot] = wv[...]

            @pl.when(jnp.logical_not(mine))
            def _():
                rcopy(wv, wp.at[w_slot], w_send.at[0], w_recv.at[0], *place(x, rem(y + i, 8), z, w_core))

    def cross_w(n):
        some = wp.at[pl.ds(8 * xl + 4 * n, 4)]
        rcopy(some, some, w_send.at[1], w_recv.at[1], *place(2 * xh + 1 - xl, y, z, k))

    introduce()
    spread_w()
    pending.append(lambda: wait_some(wp.at[pl.ds(0, 8)], w_send.at[0], w_kept))

    def squares(r):
        v = xb[r, :].astype(F32)
        s = jnp.sum(v * v, axis=0, keepdims=True)
        t = s[:, 0:128]
        for i in range(1, 16):
            t = t + s[:, i * 128:(i + 1) * 128]
        return t

    total = jnp.zeros((1, 128), F32)
    for ch in range(CH):
        total = total + squares(rows(own, ch))
    for ch in range(CH):
        for j in range(3):
            r = rows(own + 1 + j, ch)
            wait_bytes(xb.at[r], ag_recv.at[j, ch])
            rcopy(xb.at[r], xb.at[r], fw_send, fw_recv, partner, m)
        for j in range(3):
            total = total + squares(rows(own + 1 + j, ch))
    ss[...] = total
    rcopy(ss, sso, ss_sem.at[0], ss_sem.at[1], partner, m)
    pending.append(lambda: wait_bytes(ss, ss_sem.at[0]))
    wait_bytes(xb.at[pl.ds(0, 512)], fw_recv)

    def cols(i):
        return xb[:, pl.ds(pl.multiple_of(i * 128, 128), 128)]

    first_slot = z * (1 - k) + y * k
    second_slot = y * (1 - k) + z * k
    in_half = div(y, 4) == k
    on_low = k == 0

    @pl.loop(0, 2)
    def _(parity):
        @pl.loop(0, 2)
        def _(turn):
            q = parity + 2 * turn
            m0 = 8 * k + rem(role + 4 - q, 4)
            left = jnp.concatenate([cols(m0), cols(m0 + 4)], axis=1)
            zs = [rem(q, 2) + 2 * t for t in range(4)]
            cs = [2 * zt + rem(div(q + 8 - zt, 2), 2) for zt in zs]
            right = jnp.concatenate([cols(ct) for ct in cs], axis=1)
            part = lax.dot_general(left, right, (((0,), (0,)), ((), ())),
                                   preferred_element_type=F32).astype(BF16)
            for a in range(2):
                yo = div(m0 + 4 * a, 2) - 4 * k
                for t in range(4):
                    tile = part[a * 128:(a + 1) * 128, t * 128:(t + 1) * 128]
                    sb[0, zs[t] * 4 + yo] = tile[:64]
                    sb[1, yo * 8 + zs[t]] = tile[64:]

        @pl.loop(1, 9)
        def _(i):
            xx, yy, zz = diagonal(0, i)
            dg, dm = place(xx, yy, zz, 0)
            piece = sb.at[0, pl.ds(zz * 4, 4)]
            there = pl.ds(z * 8 + 4 * k, 4)
            ready = rem(zz, 2) == parity
            mine = jnp.logical_and(ready, jnp.logical_and(on_low, i == 8))

            @pl.when(mine)
            def _():
                ra[there] = piece[...]

            @pl.when(jnp.logical_and(ready, jnp.logical_not(jnp.logical_and(on_low, i == 8))))
            def _():
                rcopy(piece, ra.at[there], rs_send.at[0], rs_recv, dg, dm)

    @pl.loop(1, 5)
    def _(i):
        yo = rem(y + i, 4)
        yy = 4 * k + yo
        xx = rem(role + 24 - 2 * yy - z, 4)
        dg, dm = place(xx, yy, z, 1)
        piece = sb.at[1, pl.ds(yo * 8, 8)]
        there = pl.ds(y * 8, 8)
        mine = jnp.logical_and(k == 1, yy == y)

        @pl.when(mine)
        def _():
            ra[there] = piece[...]

        @pl.when(jnp.logical_not(mine))
        def _():
            rcopy(piece, ra.at[there], rs_send.at[1], rs_recv, dg, dm)

    wait_bytes(sso, ss_sem.at[1])
    ssx[...] = ss[...] + sso[...]
    ssa[first_slot] = ssx[...]

    @pl.loop(1, 8)
    def _(i):
        dg, dm = place(*diagonal(k * i, (1 - k) * i), k)
        rcopy(ssx, ssa.at[first_slot], sr_send.at[0], sr_recv.at[0], dg, dm)

    def wait_first(sem, sending):
        full = sb.at[0]
        if sending:
            pl.when(on_low)(lambda: wait_bytes(full.at[pl.ds(0, 28)], sem.at[0]))
            pl.when(k == 1)(lambda: wait_bytes(full, sem.at[0]))
            kept = jnp.logical_and(k == 1, in_half)
            pl.when(kept)(lambda: wait_bytes(full.at[pl.ds(0, 24)], sem.at[1]))
            pl.when(jnp.logical_not(kept))(lambda: wait_bytes(full, sem.at[1]))
        else:
            kept = jnp.logical_and(k == 1, in_half)
            pl.when(on_low)(lambda: wait_bytes(ra.at[pl.ds(0, 60)], sem))
            pl.when(kept)(lambda: wait_bytes(ra.at[pl.ds(0, 56)], sem))
            pl.when(jnp.logical_and(k == 1, jnp.logical_not(in_half)))(lambda: wait_bytes(ra, sem))

    pending.append(lambda: wait_first(rs_send, True))
    pending.append(lambda: wait_bytes(ssa.at[pl.ds(0, 7)], sr_send.at[0]))
    wait_first(rs_recv, False)
    wait_bytes(ssa.at[pl.ds(0, 7)], sr_recv.at[0])
    ssy[...] = jnp.sum(ssa[...], axis=0)

    @pl.loop(1, 9)
    def _(i):
        to = rem(second_slot + i, 8)
        acc = ra[to].astype(F32)
        for j in range(1, 8):
            acc = acc + ra[j * 8 + to].astype(F32)
        dg, dm = place(*diagonal((1 - k) * i, k * i), k)

        @pl.when(i == 8)
        def _():
            rb[second_slot] = acc
            ssb[second_slot] = ssy[...]

        @pl.when(i < 8)
        def _():
            sb2[to] = acc
            rcopy(sb2.at[to], rb.at[second_slot], rs2_send, rs2_recv, dg, dm)
            rcopy(ssy, ssb.at[second_slot], sr_send.at[1], sr_recv.at[1], dg, dm)

    pending.append(lambda: wait_bytes(rb.at[pl.ds(0, 7)], rs2_send))
    pending.append(lambda: wait_bytes(ssb.at[pl.ds(0, 7)], sr_send.at[1]))
    wait_bytes(rb.at[pl.ds(0, 7)], rs2_recv)
    wait_bytes(ssb.at[pl.ds(0, 7)], sr_recv.at[1])
    cov = rb[0]
    for j in range(1, 8):
        cov = cov + rb[j]
    total_sq = jnp.sum(ssb[...])
    scale = 2048.0 / (6.0 * total_sq)
    it = cov * scale
    row_core, col_core = div(c, 8), div(m, 8)
    row_slot = 2 * rem(c, 8) + k
    col_slot = 2 * rem(m, 8) + k
    own_row, own_col = row_core == k, col_core == k

    def along_row(src, dst, n):
        @pl.loop(0, 16)
        def _(i):
            dg = 2 * rem(c + i, 16) + row_core

            @pl.when(dg == g)
            def _():
                dst[row_slot] = src[...]

            @pl.when(dg != g)
            def _():
                rcopy(src, dst.at[row_slot], row_send.at[n], row_recv.at[n], dg, m)

    def along_col(src, dst, n):
        @pl.loop(0, 16)
        def _(i):
            dg, dm = 2 * c + col_core, rem(m + i, 16)
            mine = jnp.logical_and(dg == g, dm == m)

            @pl.when(mine)
            def _():
                dst[col_slot] = src[...]

            @pl.when(jnp.logical_not(mine))
            def _():
                rcopy(src, dst.at[col_slot], col_send.at[n], col_recv.at[n], dg, dm)

    def side_by_side(ref):
        return jnp.concatenate(
            [ref[2 * j:2 * j + 2].reshape(128, 128) for j in range(8)], axis=1)

    def tile_product(lp, rp, out, got, n):
        out[...] = jnp.dot(side_by_side(lp), rp[...].reshape(1024, 128),
                           preferred_element_type=F32)
        other = pl.ds(pl.multiple_of(64 * (1 - k), 64), 64)
        rcopy(out.at[other], got, ex_send.at[n], ex_recv.at[n], partner, m)
        mine = out[pl.ds(pl.multiple_of(64 * k, 64), 64), :]
        wait_bytes(got, ex_recv.at[n])
        return mine + got[...]

    it16 = it.astype(BF16)
    yb[...] = it16
    along_row(yb, rowp, 0)
    along_col(yb, colp, 0)
    wait_some(wp.at[pl.ds(0, 8)], w_recv.at[0], w_kept)
    cross_w(0)
    pending.append(lambda: wait_some(rowp, row_send.at[0], own_row))
    pending.append(lambda: wait_some(colp, col_send.at[0], own_col))
    wait_some(rowp, row_recv.at[0], own_row)
    wait_some(colp, col_recv.at[0], own_col)
    sq = tile_product(rowp, colp, exs, exr, 0)
    pending.append(lambda: wait_bytes(exr, ex_send.at[0]))

    sq16 = sq.astype(BF16)
    ab[...] = sq16
    bb[...] = (0.0625 * sq - 0.5625 * it).astype(BF16)
    along_row(ab, rowp2, 1)
    along_col(bb, colp2, 1)
    cross_w(1)
    pending.append(lambda: wait_bytes(wp.at[pl.ds(0, 8)], w_send.at[1]))
    pending.append(lambda: wait_some(rowp2, row_send.at[1], own_row))
    pending.append(lambda: wait_some(colp2, col_send.at[1], own_col))
    wait_some(rowp2, row_recv.at[1], own_row)
    wait_some(colp2, col_recv.at[1], own_col)
    higher = tile_product(rowp2, colp2, exs2, exr2, 1)
    pending.append(lambda: wait_bytes(exr2, ex_send.at[1]))

    row_ids = m * 128 + 64 * k + lax.broadcasted_iota(jnp.int32, (64, 128), 0)
    col_ids = c * 128 + lax.broadcasted_iota(jnp.int32, (64, 128), 1)
    unit = jnp.where(row_ids == col_ids, 2.25, 0.0).astype(F32)
    zz_tile = unit - 2.4375 * it + 1.6875 * sq + higher
    qb[...] = (higher - 2.4375 * (it - it16.astype(F32)) + 1.6875 * (sq - sq16.astype(F32))).astype(BF16)
    along_row(qb, qp, 2)
    zb[...] = zz_tile
    rcopy(zb, zx, ex_send.at[2], ex_recv.at[2], partner, m)
    pending.append(lambda: wait_some(qp, row_send.at[2], own_row))
    pending.append(lambda: wait_bytes(zx, ex_send.at[2]))

    wait_bytes(zx, ex_recv.at[2])
    whole_tile[pl.ds(pl.multiple_of(64 * k, 64), 64), :] = zb[...]
    whole_tile[pl.ds(pl.multiple_of(64 * (1 - k), 64), 64), :] = zx[...]
    whole_tile[...] = whole_tile[...].T
    root_ref[...] = whole_tile[pl.ds(pl.multiple_of(64 * k, 64), 64), :]

    wait_bytes(wp.at[pl.ds(0, 8)], w_recv.at[1])
    left = 1.6875 * side_by_side(rowp2).astype(F32) - 2.4375 * side_by_side(rowp).astype(F32)
    hi = left.astype(BF16)
    lo = (left - hi.astype(F32)).astype(BF16)

    def weighted(kk, parts):
        cols_kk = jnp.concatenate(
            [wp[8 * (j % 2) + 2 * (j // 2) + kk] for j in range(8)], axis=1)
        return sum(lax.dot_general(cols_kk, p, (((1,), (1,)), ((), ())),
                                   preferred_element_type=F32) for p in parts)

    cxs[...] = weighted(1 - k, (hi, lo))
    cond_ref[...] = weighted(k, (hi, lo)) + 2.25 * wv[...].astype(F32)
    wait_some(qp, row_recv.at[2], own_row)
    rest = side_by_side(qp)
    cxs[...] += weighted(1 - k, (rest,))
    rcopy(cxs, cxr, ex_send.at[3], ex_recv.at[3], partner, m)
    pending.append(lambda: wait_bytes(cxr, ex_send.at[3]))
    cond_ref[...] += weighted(k, (rest,))
    wait_bytes(cxr, ex_recv.at[3])
    cond_ref[...] += cxr[...]

    for finish in pending:
        finish()


def on_device(hidden_grads, weight_grad):
    dma = pltpu.SemaphoreType.DMA
    vm = pltpu.VMEM
    root, conditioned = pl.pallas_call(
        kernel,
        out_shape=(jax.ShapeDtypeStruct((64, 128), F32), jax.ShapeDtypeStruct((192, 128), F32)),
        in_specs=[pl.BlockSpec(memory_space=pltpu.HBM)] * 2,
        out_specs=(pl.BlockSpec(memory_space=pltpu.VMEM),) * 2,
        scratch_shapes=[
            vm((1024, 2048), BF16),
            vm((192, 128), BF16),
            vm((2, 32, 64, 128), BF16),
            vm((64, 64, 128), BF16),
            vm((8, 64, 128), F32), vm((8, 64, 128), F32),
            vm((1, 128), F32), vm((1, 128), F32), vm((1, 128), F32),
            vm((8, 1, 128), F32), vm((1, 128), F32), vm((8, 1, 128), F32),
            vm((64, 128), BF16),
            vm((16, 64, 128), BF16), vm((16, 64, 128), BF16),
            vm((128, 128), F32), vm((64, 128), F32),
            vm((64, 128), BF16), vm((64, 128), BF16),
            vm((16, 64, 128), BF16), vm((16, 64, 128), BF16),
            vm((128, 128), F32), vm((64, 128), F32),
            vm((64, 128), F32), vm((64, 128), F32), vm((128, 128), F32),
            vm((64, 128), BF16), vm((16, 64, 128), BF16),
            vm((16, 192, 128), BF16),
            vm((192, 128), F32), vm((192, 128), F32),
            dma((2,)), dma, dma((3, CH)), dma, dma, dma((2,)), dma((2,)), dma,
            dma, dma, dma((2,)), dma((2,)), dma((3,)), dma((3,)), dma((2,)), dma((2,)), dma((4,)), dma((4,)),
            dma((2,)), dma((2,)), pltpu.SemaphoreType.REGULAR((4,)),
        ],
        compiler_params=pltpu.CompilerParams(has_side_effects=True, collective_id=0, vmem_limit_bytes=66700000),
        name="kfac",
    )(hidden_grads, weight_grad.T)
    return root.T, conditioned.T


def solution(mesh):
    spec = P("mem", "grp")
    return jax.shard_map(
        on_device,
        mesh=mesh,
        in_specs=(P(("grp", "mem"), None), spec),
        out_specs=(spec, spec),
        check_vma=False,
    )
```

```python
import functools

import jax
import jax.numpy as jnp
from jax import lax
from jax.experimental import pallas as pl
from jax.experimental.pallas import tpu as pltpu
from jax.sharding import PartitionSpec as P

MESH = pl.DeviceIdType.MESH
F32 = jnp.float32
BF16 = jnp.bfloat16
CH = 4
ROWS = 128 // CH
rem = lax.rem
div = lax.div


def rcopy(src, dst, ssem, rsem, g, m):
    cp = pltpu.make_async_remote_copy(
        src_ref=src, dst_ref=dst, send_sem=ssem, recv_sem=rsem,
        device_id=(g, m), device_id_type=MESH,
    )
    cp.start()


def far_first(t):
    return 4 + div(t + 1, 2) * (1 - 2 * rem(t, 2))


def wait_bytes(ref, sem):
    pltpu.make_async_copy(ref, ref, sem).wait()


def wait_some(ref, sem, fewer):
    @pl.when(fewer)
    def _():
        wait_bytes(ref.at[pl.ds(0, ref.shape[0] - 1)], sem)

    @pl.when(jnp.logical_not(fewer))
    def _():
        wait_bytes(ref, sem)


def kernel(
    x_hbm, w_hbm, root_ref, cond_ref,
    xb, wv, sb, ra, sb2, rb, ss, sso, ssx, ssa, ssy, ssb, yb, rowp, colp, exs, exr,
    ab, bb, rowp2, colp2, exs2, exr2, zb, zx, whole_tile, qb, qp, wp, cxs, cxr,
    lsem, ag_send, ag_recv, fw_send, fw_recv, ss_sem, rs_send, rs_recv, rs2_send, rs2_recv,
    sr_send, sr_recv, row_send, row_recv, col_send, col_recv, ex_send, ex_recv,
    w_send, w_recv, met,
):
    g = lax.axis_index("grp")
    m = lax.axis_index("mem")
    k, c = rem(g, 2), div(g, 2)
    z, xh = div(c, 2), rem(c, 2)
    y, xl = div(m, 2), rem(m, 2)
    x = 2 * xh + xl
    role = rem(x + 2 * y + z, 4)
    partner = c * 2 + 1 - k

    def place(xx, yy, zz, kk):
        return (zz * 2 + div(xx, 2)) * 2 + kk, yy * 2 + rem(xx, 2)

    own = 4 * k
    load_x = pltpu.make_async_copy(x_hbm, xb.at[pl.ds(own * 128, 128)], lsem.at[0])
    load_w = pltpu.make_async_copy(w_hbm, wv, lsem.at[1])
    load_x.start()
    load_w.start()

    barrier = pltpu.get_barrier_semaphore()

    def greet(dg, dm):
        pl.semaphore_signal(barrier, inc=1, device_id=(dg, dm), device_id_type=MESH)

    def diagonal(dy, dz):
        yy, zz = rem(y + dy, 8), rem(z + dz, 8)
        return rem(role + 24 - 2 * yy - zz, 4), yy, zz

    greet(partner, m)
    for step in (1, 7):
        greet(*place(rem(x + step, 4), y, z, k))
        greet(*place(x, rem(y + step, 8), z, k))
        greet(*place(x, y, rem(z + step, 8), k))
    pl.semaphore_wait(barrier, 7)

    def introduce():
        def nudge(n, dg, dm):
            pl.semaphore_signal(met.at[n], inc=1, device_id=(dg, dm), device_id_type=MESH)

        for step in (1, 3):
            nudge(0, *place(rem(x + step, 4), y, z, k))
        pl.semaphore_wait(met.at[0], 2)
        for n, steps in ((1, (1, 7)), (2, (2, 6))):
            for step in steps:
                nudge(n, *place(x, rem(y + step, 8), z, k))
                nudge(n, *place(x, y, rem(z + step, 8), k))
            pl.semaphore_wait(met.at[n], 4)
        nudge(3, partner, m)
        pl.semaphore_wait(met.at[3], 1)

    def rows(slot, ch):
        return pl.ds(pl.multiple_of(slot * 128 + ch * ROWS, ROWS), ROWS)

    def diagonal(dy, dz):
        yy, zz = rem(y + dy, 8), rem(z + dz, 8)
        return rem(role + 24 - 2 * yy - zz, 4), yy, zz

    pending = []

    load_x.wait()
    near = (
        place(rem(x + 1 - k, 4), y, rem(z + k, 8), k),
        place(rem(x + 3 * (1 - k), 4), y, rem(z + 7 * k, 8), k),
        place(x, rem(y + 1 + 6 * k, 8), z, k),
    )
    for ch in range(CH):
        for j in range(3):
            rcopy(xb.at[rows(own, ch)], xb.at[rows(own + 1 + j, ch)],
                  ag_send, ag_recv.at[j, ch], *near[j])
    whole = pl.ds(pl.multiple_of(own * 128, 128), 128)
    rcopy(xb.at[whole], xb.at[whole], fw_send, fw_recv, partner, m)
    pending.append(lambda: wait_bytes(xb.at[pl.ds(0, 384)], ag_send))
    pending.append(lambda: wait_bytes(xb.at[pl.ds(0, 512)], fw_send))

    load_w.wait()
    w_slot = 8 * xl + 2 * rem(y, 4) + k
    w_core = div(y, 4)
    w_kept = w_core == k

    def spread_w():
        @pl.loop(1, 9)
        def _(i):
            mine = jnp.logical_and(i == 8, w_kept)

            @pl.when(mine)
            def _():
                wp[w_slot] = wv[...]

            @pl.when(jnp.logical_not(mine))
            def _():
                rcopy(wv, wp.at[w_slot], w_send.at[0], w_recv.at[0], *place(x, rem(y + i, 8), z, w_core))

    def cross_w(n):
        some = wp.at[pl.ds(8 * xl + 4 * n, 4)]
        rcopy(some, some, w_send.at[1], w_recv.at[1], *place(2 * xh + 1 - xl, y, z, k))

    introduce()
    spread_w()
    pending.append(lambda: wait_some(wp.at[pl.ds(0, 8)], w_send.at[0], w_kept))

    def squares(r):
        v = xb[r, :].astype(F32)
        s = jnp.sum(v * v, axis=0, keepdims=True)
        t = s[:, 0:128]
        for i in range(1, 16):
            t = t + s[:, i * 128:(i + 1) * 128]
        return t

    total = jnp.zeros((1, 128), F32)
    for ch in range(CH):
        total = total + squares(rows(own, ch))
    for ch in range(CH):
        for j in range(3):
            r = rows(own + 1 + j, ch)
            wait_bytes(xb.at[r], ag_recv.at[j, ch])
            rcopy(xb.at[r], xb.at[r], fw_send, fw_recv, partner, m)
        for j in range(3):
            total = total + squares(rows(own + 1 + j, ch))
    ss[...] = total
    rcopy(ss, sso, ss_sem.at[0], ss_sem.at[1], partner, m)
    pending.append(lambda: wait_bytes(ss, ss_sem.at[0]))
    wait_bytes(xb.at[pl.ds(0, 512)], fw_recv)

    def cols(i):
        return xb[:, pl.ds(pl.multiple_of(i * 128, 128), 128)]

    first_slot = z * (1 - k) + y * k
    second_slot = y * (1 - k) + z * k
    in_half = div(y, 4) == k
    on_low = k == 0

    @pl.loop(0, 2)
    def _(parity):
        @pl.loop(0, 2)
        def _(turn):
            q = parity + 2 * turn
            m0 = 8 * k + rem(role + 4 - q, 4)
            left = jnp.concatenate([cols(m0), cols(m0 + 4)], axis=1)
            zs = [rem(q, 2) + 2 * t for t in range(4)]
            cs = [2 * zt + rem(div(q + 8 - zt, 2), 2) for zt in zs]
            right = jnp.concatenate([cols(ct) for ct in cs], axis=1)
            part = lax.dot_general(left, right, (((0,), (0,)), ((), ())),
                                   preferred_element_type=F32).astype(BF16)
            for a in range(2):
                yo = div(m0 + 4 * a, 2) - 4 * k
                for t in range(4):
                    tile = part[a * 128:(a + 1) * 128, t * 128:(t + 1) * 128]
                    sb[0, zs[t] * 4 + yo] = tile[:64]
                    sb[1, yo * 8 + zs[t]] = tile[64:]

        @pl.loop(0, 8)
        def _(t):
            i = far_first(t)
            xx, yy, zz = diagonal(0, i)
            dg, dm = place(xx, yy, zz, 0)
            piece = sb.at[0, pl.ds(zz * 4, 4)]
            there = pl.ds(z * 8 + 4 * k, 4)
            ready = rem(zz, 2) == parity
            mine = jnp.logical_and(ready, jnp.logical_and(on_low, i == 0))

            @pl.when(mine)
            def _():
                ra[there] = piece[...]

            @pl.when(jnp.logical_and(ready, jnp.logical_not(jnp.logical_and(on_low, i == 0))))
            def _():
                rcopy(piece, ra.at[there], rs_send.at[0], rs_recv, dg, dm)

    @pl.loop(1, 5)
    def _(i):
        yo = rem(y + i, 4)
        yy = 4 * k + yo
        xx = rem(role + 24 - 2 * yy - z, 4)
        dg, dm = place(xx, yy, z, 1)
        piece = sb.at[1, pl.ds(yo * 8, 8)]
        there = pl.ds(y * 8, 8)
        mine = jnp.logical_and(k == 1, yy == y)

        @pl.when(mine)
        def _():
            ra[there] = piece[...]

        @pl.when(jnp.logical_not(mine))
        def _():
            rcopy(piece, ra.at[there], rs_send.at[1], rs_recv, dg, dm)

    wait_bytes(sso, ss_sem.at[1])
    ssx[...] = ss[...] + sso[...]
    ssa[first_slot] = ssx[...]

    @pl.loop(1, 8)
    def _(i):
        dg, dm = place(*diagonal(k * i, (1 - k) * i), k)
        rcopy(ssx, ssa.at[first_slot], sr_send.at[0], sr_recv.at[0], dg, dm)

    def wait_first(sem, sending):
        full = sb.at[0]
        if sending:
            pl.when(on_low)(lambda: wait_bytes(full.at[pl.ds(0, 28)], sem.at[0]))
            pl.when(k == 1)(lambda: wait_bytes(full, sem.at[0]))
            kept = jnp.logical_and(k == 1, in_half)
            pl.when(kept)(lambda: wait_bytes(full.at[pl.ds(0, 24)], sem.at[1]))
            pl.when(jnp.logical_not(kept))(lambda: wait_bytes(full, sem.at[1]))
        else:
            kept = jnp.logical_and(k == 1, in_half)
            pl.when(on_low)(lambda: wait_bytes(ra.at[pl.ds(0, 60)], sem))
            pl.when(kept)(lambda: wait_bytes(ra.at[pl.ds(0, 56)], sem))
            pl.when(jnp.logical_and(k == 1, jnp.logical_not(in_half)))(lambda: wait_bytes(ra, sem))

    pending.append(lambda: wait_first(rs_send, True))
    pending.append(lambda: wait_bytes(ssa.at[pl.ds(0, 7)], sr_send.at[0]))
    wait_first(rs_recv, False)
    wait_bytes(ssa.at[pl.ds(0, 7)], sr_recv.at[0])
    ssy[...] = jnp.sum(ssa[...], axis=0)

    @pl.loop(0, 8)
    def _(t):
        i = far_first(t)
        to = rem(second_slot + i, 8)
        acc = ra[to].astype(F32)
        for j in range(1, 8):
            acc = acc + ra[j * 8 + to].astype(F32)
        dg, dm = place(*diagonal((1 - k) * i, k * i), k)

        @pl.when(i == 0)
        def _():
            rb[second_slot] = acc
            ssb[second_slot] = ssy[...]

        @pl.when(i > 0)
        def _():
            sb2[to] = acc
            rcopy(sb2.at[to], rb.at[second_slot], rs2_send, rs2_recv, dg, dm)
            rcopy(ssy, ssb.at[second_slot], sr_send.at[1], sr_recv.at[1], dg, dm)

    pending.append(lambda: wait_bytes(rb.at[pl.ds(0, 7)], rs2_send))
    pending.append(lambda: wait_bytes(ssb.at[pl.ds(0, 7)], sr_send.at[1]))
    wait_bytes(rb.at[pl.ds(0, 7)], rs2_recv)
    wait_bytes(ssb.at[pl.ds(0, 7)], sr_recv.at[1])
    cov = rb[0]
    for j in range(1, 8):
        cov = cov + rb[j]
    total_sq = jnp.sum(ssb[...])
    scale = 2048.0 / (6.0 * total_sq)
    it = cov * scale
    row_core, col_core = div(c, 8), div(m, 8)
    row_slot = 2 * rem(c, 8) + k
    col_slot = 2 * rem(m, 8) + k
    own_row, own_col = row_core == k, col_core == k

    def along_row(src, dst, n, ordered=False):
        @pl.loop(0, 16)
        def _(t):
            dx = 1 - rem(t, 2)
            to = div(t, 2) if ordered else rem(z + far_first(div(t, 2)), 8)
            dg = 2 * (2 * to + rem(xh + dx, 2)) + row_core

            @pl.when(dg == g)
            def _():
                dst[row_slot] = src[...]

            @pl.when(dg != g)
            def _():
                rcopy(src, dst.at[row_slot], row_send.at[n], row_recv.at[n], dg, m)

    def along_col(src, dst, n):
        @pl.loop(0, 16)
        def _(t):
            dy, dx = far_first(div(t, 2)), 1 - rem(t, 2)
            dg, dm = 2 * c + col_core, 2 * rem(y + dy, 8) + rem(xl + dx, 2)
            mine = jnp.logical_and(dg == g, dm == m)

            @pl.when(mine)
            def _():
                dst[col_slot] = src[...]

            @pl.when(jnp.logical_not(mine))
            def _():
                rcopy(src, dst.at[col_slot], col_send.at[n], col_recv.at[n], dg, dm)

    def side_by_side(ref):
        return jnp.concatenate(
            [ref[2 * j:2 * j + 2].reshape(128, 128) for j in range(8)], axis=1)

    def tile_product(lp, rp, out, got, n):
        out[...] = jnp.dot(side_by_side(lp), rp[...].reshape(1024, 128),
                           preferred_element_type=F32)
        other = pl.ds(pl.multiple_of(64 * (1 - k), 64), 64)
        rcopy(out.at[other], got, ex_send.at[n], ex_recv.at[n], partner, m)
        mine = out[pl.ds(pl.multiple_of(64 * k, 64), 64), :]
        wait_bytes(got, ex_recv.at[n])
        return mine + got[...]

    it16 = it.astype(BF16)
    yb[...] = it16
    along_row(yb, rowp, 0)
    along_col(yb, colp, 0)
    wait_some(wp.at[pl.ds(0, 8)], w_recv.at[0], w_kept)
    cross_w(0)
    pending.append(lambda: wait_some(rowp, row_send.at[0], own_row))
    pending.append(lambda: wait_some(colp, col_send.at[0], own_col))
    wait_some(rowp, row_recv.at[0], own_row)
    wait_some(colp, col_recv.at[0], own_col)
    sq = tile_product(rowp, colp, exs, exr, 0)
    pending.append(lambda: wait_bytes(exr, ex_send.at[0]))

    sq16 = sq.astype(BF16)
    ab[...] = sq16
    bb[...] = (0.0625 * sq - 0.5625 * it).astype(BF16)
    along_row(ab, rowp2, 1)
    along_col(bb, colp2, 1)
    cross_w(1)
    pending.append(lambda: wait_bytes(wp.at[pl.ds(0, 8)], w_send.at[1]))
    pending.append(lambda: wait_some(rowp2, row_send.at[1], own_row))
    pending.append(lambda: wait_some(colp2, col_send.at[1], own_col))
    wait_some(rowp2, row_recv.at[1], own_row)
    wait_some(colp2, col_recv.at[1], own_col)
    higher = tile_product(rowp2, colp2, exs2, exr2, 1)
    pending.append(lambda: wait_bytes(exr2, ex_send.at[1]))

    row_ids = m * 128 + 64 * k + lax.broadcasted_iota(jnp.int32, (64, 128), 0)
    col_ids = c * 128 + lax.broadcasted_iota(jnp.int32, (64, 128), 1)
    unit = jnp.where(row_ids == col_ids, 2.25, 0.0).astype(F32)
    zz_tile = unit - 2.4375 * it + 1.6875 * sq + higher
    qb[...] = (higher - 2.4375 * (it - it16.astype(F32)) + 1.6875 * (sq - sq16.astype(F32))).astype(BF16)
    along_row(qb, qp, 2, ordered=True)
    zb[...] = zz_tile
    rcopy(zb, zx, ex_send.at[2], ex_recv.at[2], partner, m)
    pending.append(lambda: wait_some(qp, row_send.at[2], own_row))
    pending.append(lambda: wait_bytes(zx, ex_send.at[2]))

    wait_bytes(zx, ex_recv.at[2])
    whole_tile[pl.ds(pl.multiple_of(64 * k, 64), 64), :] = zb[...]
    whole_tile[pl.ds(pl.multiple_of(64 * (1 - k), 64), 64), :] = zx[...]
    whole_tile[...] = whole_tile[...].T
    root_ref[...] = whole_tile[pl.ds(pl.multiple_of(64 * k, 64), 64), :]

    wait_bytes(wp.at[pl.ds(0, 8)], w_recv.at[1])
    left = 1.6875 * side_by_side(rowp2).astype(F32) - 2.4375 * side_by_side(rowp).astype(F32)
    hi = left.astype(BF16)
    lo = (left - hi.astype(F32)).astype(BF16)

    def weighted(kk, parts):
        cols_kk = jnp.concatenate(
            [wp[8 * (j % 2) + 2 * (j // 2) + kk] for j in range(8)], axis=1)
        return sum(lax.dot_general(cols_kk, p, (((1,), (1,)), ((), ())),
                                   preferred_element_type=F32) for p in parts)

    cxs[...] = weighted(1 - k, (hi, lo))
    cond_ref[...] = weighted(k, (hi, lo)) + 2.25 * wv[...].astype(F32)
    wait_some(qp, row_recv.at[2], own_row)
    rest = side_by_side(qp)
    cxs[...] += weighted(1 - k, (rest,))
    rcopy(cxs, cxr, ex_send.at[3], ex_recv.at[3], partner, m)
    pending.append(lambda: wait_bytes(cxr, ex_send.at[3]))
    cond_ref[...] += weighted(k, (rest,))
    wait_bytes(cxr, ex_recv.at[3])
    cond_ref[...] += cxr[...]

    for finish in pending:
        finish()


def on_device(hidden_grads, weight_grad):
    dma = pltpu.SemaphoreType.DMA
    vm = pltpu.VMEM
    root, conditioned = pl.pallas_call(
        kernel,
        out_shape=(jax.ShapeDtypeStruct((64, 128), F32), jax.ShapeDtypeStruct((192, 128), F32)),
        in_specs=[pl.BlockSpec(memory_space=pltpu.HBM)] * 2,
        out_specs=(pl.BlockSpec(memory_space=pltpu.VMEM),) * 2,
        scratch_shapes=[
            vm((1024, 2048), BF16),
            vm((192, 128), BF16),
            vm((2, 32, 64, 128), BF16),
            vm((64, 64, 128), BF16),
            vm((8, 64, 128), F32), vm((8, 64, 128), F32),
            vm((1, 128), F32), vm((1, 128), F32), vm((1, 128), F32),
            vm((8, 1, 128), F32), vm((1, 128), F32), vm((8, 1, 128), F32),
            vm((64, 128), BF16),
            vm((16, 64, 128), BF16), vm((16, 64, 128), BF16),
            vm((128, 128), F32), vm((64, 128), F32),
            vm((64, 128), BF16), vm((64, 128), BF16),
            vm((16, 64, 128), BF16), vm((16, 64, 128), BF16),
            vm((128, 128), F32), vm((64, 128), F32),
            vm((64, 128), F32), vm((64, 128), F32), vm((128, 128), F32),
            vm((64, 128), BF16), vm((16, 64, 128), BF16),
            vm((16, 192, 128), BF16),
            vm((192, 128), F32), vm((192, 128), F32),
            dma((2,)), dma, dma((3, CH)), dma, dma, dma((2,)), dma((2,)), dma,
            dma, dma, dma((2,)), dma((2,)), dma((3,)), dma((3,)), dma((2,)), dma((2,)), dma((4,)), dma((4,)),
            dma((2,)), dma((2,)), pltpu.SemaphoreType.REGULAR((4,)),
        ],
        compiler_params=pltpu.CompilerParams(has_side_effects=True, collective_id=0, vmem_limit_bytes=56000000),
        name="kfac",
    )(hidden_grads, weight_grad.T)
    return root.T, conditioned.T


def solution(mesh):
    spec = P("mem", "grp")
    return jax.shard_map(
        on_device,
        mesh=mesh,
        in_specs=(P(("grp", "mem"), None), spec),
        out_specs=(spec, spec),
        check_vma=False,
    )
```

```python
import functools

import jax
import jax.numpy as jnp
from jax import lax
from jax.experimental import pallas as pl
from jax.experimental.pallas import tpu as pltpu
from jax.sharding import PartitionSpec as P

MESH = pl.DeviceIdType.MESH
F32 = jnp.float32
BF16 = jnp.bfloat16
CH = 8
ROWS = 128 // CH
rem = lax.rem
div = lax.div


def rcopy(src, dst, ssem, rsem, g, m):
    cp = pltpu.make_async_remote_copy(
        src_ref=src, dst_ref=dst, send_sem=ssem, recv_sem=rsem,
        device_id=(g, m), device_id_type=MESH,
    )
    cp.start()


FAR_FIRST = (4, 3, 5, 2, 6, 1, 7, 0)


def wait_bytes(ref, sem):
    pltpu.make_async_copy(ref, ref, sem).wait()


def wait_some(ref, sem, fewer):
    @pl.when(fewer)
    def _():
        wait_bytes(ref.at[pl.ds(0, ref.shape[0] - 1)], sem)

    @pl.when(jnp.logical_not(fewer))
    def _():
        wait_bytes(ref, sem)


def kernel(
    x_hbm, w_hbm, root_ref, cond_ref,
    xb, wv, sb, ra, sb2, rb, ss, sso, ssx, ssa, ssy, ssb, yb, rowp, colp, exs, exr,
    ab, bb, rowp2, colp2, exs2, exr2, zb, zx, whole_tile, qb, qp, wp, cxs, cxr,
    lsem, ag_send, ag_recv, fw_send, fw_recv, ss_sem, rs_send, rs_recv, rs2_send, rs2_recv,
    sr_send, sr_recv, row_send, row_recv, col_send, col_recv, ex_send, ex_recv,
    w_send, w_recv, met,
):
    g = lax.axis_index("grp")
    m = lax.axis_index("mem")
    k, c = rem(g, 2), div(g, 2)
    z, xh = div(c, 2), rem(c, 2)
    y, xl = div(m, 2), rem(m, 2)
    x = 2 * xh + xl
    role = rem(x + 2 * y + z, 4)
    partner = c * 2 + 1 - k

    def place(xx, yy, zz, kk):
        return (zz * 2 + div(xx, 2)) * 2 + kk, yy * 2 + rem(xx, 2)

    own = 4 * k
    load_x = pltpu.make_async_copy(x_hbm, xb.at[pl.ds(own * 128, 128)], lsem.at[0])
    load_w = pltpu.make_async_copy(w_hbm, wv, lsem.at[1])
    load_x.start()
    load_w.start()

    barrier = pltpu.get_barrier_semaphore()

    def greet(dg, dm):
        pl.semaphore_signal(barrier, inc=1, device_id=(dg, dm), device_id_type=MESH)

    greet(partner, m)
    for step in (1, 7):
        greet(*place(rem(x + step, 4), y, z, k))
        greet(*place(x, rem(y + step, 8), z, k))
        greet(*place(x, y, rem(z + step, 8), k))
    pl.semaphore_wait(barrier, 7)

    def introduce():
        def nudge(n, dg, dm):
            pl.semaphore_signal(met.at[n], inc=1, device_id=(dg, dm), device_id_type=MESH)

        for step in (1, 3):
            nudge(0, *place(rem(x + step, 4), y, z, k))
        pl.semaphore_wait(met.at[0], 2)
        for n, steps in ((1, (1, 7)), (2, (2, 6))):
            for step in steps:
                nudge(n, *place(x, rem(y + step, 8), z, k))
                nudge(n, *place(x, y, rem(z + step, 8), k))
            pl.semaphore_wait(met.at[n], 4)
        nudge(3, partner, m)
        pl.semaphore_wait(met.at[3], 1)

    def rows(slot, ch):
        return pl.ds(pl.multiple_of(slot * 128 + ch * ROWS, ROWS), ROWS)

    zs_at = [z] + [rem(z + i, 8) for i in range(1, 8)]
    ys_at = [y] + [rem(y + i, 8) for i in range(1, 8)]
    pending = []

    load_x.wait()
    near = (
        place(rem(x + 1 - k, 4), y, rem(z + k, 8), k),
        place(rem(x + 3 * (1 - k), 4), y, rem(z + 7 * k, 8), k),
        place(x, rem(y + 1 + 6 * k, 8), z, k),
    )
    for ch in range(CH):
        for j in range(3):
            rcopy(xb.at[rows(own, ch)], xb.at[rows(own + 1 + j, ch)],
                  ag_send, ag_recv.at[j, ch], *near[j])
    whole = pl.ds(pl.multiple_of(own * 128, 128), 128)
    rcopy(xb.at[whole], xb.at[whole], fw_send, fw_recv, partner, m)
    pending.append(lambda: wait_bytes(xb.at[pl.ds(0, 384)], ag_send))
    pending.append(lambda: wait_bytes(xb.at[pl.ds(0, 512)], fw_send))

    load_w.wait()
    w_slot = 8 * xl + 2 * rem(y, 4) + k
    w_core = div(y, 4)
    w_kept = w_core == k

    def spread_w():
        for i in range(1, 8):
            rcopy(wv, wp.at[w_slot], w_send.at[0], w_recv.at[0], *place(x, ys_at[i], z, w_core))

        @pl.when(w_kept)
        def _():
            wp[w_slot] = wv[...]

        @pl.when(jnp.logical_not(w_kept))
        def _():
            rcopy(wv, wp.at[w_slot], w_send.at[0], w_recv.at[0], partner, m)

    def cross_w(n):
        some = wp.at[pl.ds(8 * xl + 4 * n, 4)]
        rcopy(some, some, w_send.at[1], w_recv.at[1], *place(2 * xh + 1 - xl, y, z, k))

    introduce()
    spread_w()
    pending.append(lambda: wait_some(wp.at[pl.ds(0, 8)], w_send.at[0], w_kept))

    def squares(r):
        v = xb[r, :].astype(F32)
        s = jnp.sum(v * v, axis=0, keepdims=True)
        t = s[:, 0:128]
        for i in range(1, 16):
            t = t + s[:, i * 128:(i + 1) * 128]
        return t

    total = jnp.zeros((1, 128), F32)
    for ch in range(CH):
        total = total + squares(rows(own, ch))
    for ch in range(CH):
        for j in range(3):
            r = rows(own + 1 + j, ch)
            wait_bytes(xb.at[r], ag_recv.at[j, ch])
            rcopy(xb.at[r], xb.at[r], fw_send, fw_recv, partner, m)
        for j in range(3):
            total = total + squares(rows(own + 1 + j, ch))
    ss[...] = total
    rcopy(ss, sso, ss_sem.at[0], ss_sem.at[1], partner, m)
    pending.append(lambda: wait_bytes(ss, ss_sem.at[0]))
    wait_bytes(xb.at[pl.ds(0, 512)], fw_recv)

    def cols(i):
        return xb[:, pl.ds(pl.multiple_of(i * 128, 128), 128)]

    first_slot = z * (1 - k) + y * k
    second_slot = y * (1 - k) + z * k
    in_half = div(y, 4) == k
    on_low = k == 0

    for odd in range(2):
        parity = rem(z + odd, 2)

        @pl.loop(0, 2)
        def _(turn, parity=parity):
            q = parity + 2 * turn
            m0 = 8 * k + rem(role + 4 - q, 4)
            left = jnp.concatenate([cols(m0), cols(m0 + 4)], axis=1)
            zs = [rem(q, 2) + 2 * t for t in range(4)]
            cs = [2 * zt + rem(div(q + 8 - zt, 2), 2) for zt in zs]
            right = jnp.concatenate([cols(ct) for ct in cs], axis=1)
            part = lax.dot_general(left, right, (((0,), (0,)), ((), ())),
                                   preferred_element_type=F32).astype(BF16)
            for a in range(2):
                yo = div(m0 + 4 * a, 2) - 4 * k
                for t in range(4):
                    tile = part[a * 128:(a + 1) * 128, t * 128:(t + 1) * 128]
                    sb[0, zs[t] * 4 + yo] = tile[:64]
                    sb[1, yo * 8 + zs[t]] = tile[64:]

        for i in FAR_FIRST:
            if i % 2 != odd:
                continue
            zz = zs_at[i]
            piece = sb.at[0, pl.ds(zz * 4, 4)]
            there = pl.ds(z * 8 + 4 * k, 4)
            if i:
                xx = rem(role + 24 - 2 * y - zz, 4)
                rcopy(piece, ra.at[there], rs_send.at[0], rs_recv, *place(xx, y, zz, 0))
                continue

            @pl.when(on_low)
            def _(piece=piece, there=there):
                ra[there] = piece[...]

            @pl.when(jnp.logical_not(on_low))
            def _(piece=piece, there=there):
                rcopy(piece, ra.at[there], rs_send.at[0], rs_recv, partner, m)

    for i in range(1, 5):
        yo = rem(y + i, 4)
        yy = 4 * k + yo
        dg, dm = place(rem(role + 24 - 2 * yy - z, 4), yy, z, 1)
        piece = sb.at[1, pl.ds(yo * 8, 8)]
        there = pl.ds(y * 8, 8)
        mine = jnp.logical_and(k == 1, yy == y)

        @pl.when(mine)
        def _(piece=piece, there=there):
            ra[there] = piece[...]

        @pl.when(jnp.logical_not(mine))
        def _(piece=piece, there=there, dg=dg, dm=dm):
            rcopy(piece, ra.at[there], rs_send.at[1], rs_recv, dg, dm)

    wait_bytes(sso, ss_sem.at[1])
    ssx[...] = ss[...] + sso[...]
    ssa[first_slot] = ssx[...]

    for i in FAR_FIRST[:7]:
        yy = (1 - k) * y + k * ys_at[i]
        zz = k * z + (1 - k) * zs_at[i]
        dg, dm = place(rem(role + 24 - 2 * yy - zz, 4), yy, zz, k)
        rcopy(ssx, ssa.at[first_slot], sr_send.at[0], sr_recv.at[0], dg, dm)

    def wait_first(sem, sending):
        full = sb.at[0]
        if sending:
            pl.when(on_low)(lambda: wait_bytes(full.at[pl.ds(0, 28)], sem.at[0]))
            pl.when(k == 1)(lambda: wait_bytes(full, sem.at[0]))
            kept = jnp.logical_and(k == 1, in_half)
            pl.when(kept)(lambda: wait_bytes(full.at[pl.ds(0, 24)], sem.at[1]))
            pl.when(jnp.logical_not(kept))(lambda: wait_bytes(full, sem.at[1]))
        else:
            kept = jnp.logical_and(k == 1, in_half)
            pl.when(on_low)(lambda: wait_bytes(ra.at[pl.ds(0, 60)], sem))
            pl.when(kept)(lambda: wait_bytes(ra.at[pl.ds(0, 56)], sem))
            pl.when(jnp.logical_and(k == 1, jnp.logical_not(in_half)))(lambda: wait_bytes(ra, sem))

    pending.append(lambda: wait_first(rs_send, True))
    pending.append(lambda: wait_bytes(ssa.at[pl.ds(0, 7)], sr_send.at[0]))
    wait_first(rs_recv, False)
    wait_bytes(ssa.at[pl.ds(0, 7)], sr_recv.at[0])
    ssy[...] = jnp.sum(ssa[...], axis=0)

    for i in FAR_FIRST:
        yy = k * y + (1 - k) * ys_at[i]
        zz = (1 - k) * z + k * zs_at[i]
        to = (1 - k) * yy + k * zz
        acc = ra[to].astype(F32)
        for j in range(1, 8):
            acc = acc + ra[j * 8 + to].astype(F32)
        if i:
            dg, dm = place(rem(role + 24 - 2 * yy - zz, 4), yy, zz, k)
            sb2[to] = acc
            rcopy(sb2.at[to], rb.at[second_slot], rs2_send, rs2_recv, dg, dm)
            rcopy(ssy, ssb.at[second_slot], sr_send.at[1], sr_recv.at[1], dg, dm)
        else:
            rb[second_slot] = acc
            ssb[second_slot] = ssy[...]

    pending.append(lambda: wait_bytes(rb.at[pl.ds(0, 7)], rs2_send))
    pending.append(lambda: wait_bytes(ssb.at[pl.ds(0, 7)], sr_send.at[1]))
    wait_bytes(rb.at[pl.ds(0, 7)], rs2_recv)
    wait_bytes(ssb.at[pl.ds(0, 7)], sr_recv.at[1])
    cov = rb[0]
    for j in range(1, 8):
        cov = cov + rb[j]
    total_sq = jnp.sum(ssb[...])
    scale = 2048.0 / (6.0 * total_sq)
    it = cov * scale
    row_core, col_core = div(c, 8), div(m, 8)
    row_slot = 2 * rem(c, 8) + k
    col_slot = 2 * rem(m, 8) + k
    own_row, own_col = row_core == k, col_core == k

    def keep_or_send(mine, src, dst, send, recv, dg, dm):
        @pl.when(mine)
        def _():
            dst[...] = src[...]

        @pl.when(jnp.logical_not(mine))
        def _():
            rcopy(src, dst, send, recv, dg, dm)

    def exchange(row_src, row_dst, col_src, col_dst, n):
        row_to, col_to = row_dst.at[row_slot], col_dst.at[col_slot]
        rs, rr, cs, cr = row_send.at[n], row_recv.at[n], col_send.at[n], col_recv.at[n]
        for i in FAR_FIRST:
            for across in (1, 0):
                xx, ww = (1 - xh, 1 - xl) if across else (xh, xl)
                rg, cg, cm = 4 * zs_at[i] + 2 * xx + row_core, 2 * c + col_core, 2 * ys_at[i] + ww
                if i or across:
                    rcopy(row_src, row_to, rs, rr, rg, m)
                    rcopy(col_src, col_to, cs, cr, cg, cm)
                else:
                    keep_or_send(own_row, row_src, row_to, rs, rr, rg, m)
                    keep_or_send(own_col, col_src, col_to, cs, cr, cg, cm)

    def along_row(src, dst, n):
        to = dst.at[row_slot]
        for zt in range(8):
            dg = 4 * zt + 2 * (1 - xh) + row_core
            rcopy(src, to, row_send.at[n], row_recv.at[n], dg, m)
            dg = 4 * zt + 2 * xh + row_core
            keep_or_send(dg == g, src, to, row_send.at[n], row_recv.at[n], dg, m)

    def side_by_side(ref):
        return jnp.concatenate(
            [ref[2 * j:2 * j + 2].reshape(128, 128) for j in range(8)], axis=1)

    def tile_product(lp, rp, out, got, n):
        out[...] = jnp.dot(side_by_side(lp), rp[...].reshape(1024, 128),
                           preferred_element_type=F32)
        other = pl.ds(pl.multiple_of(64 * (1 - k), 64), 64)
        rcopy(out.at[other], got, ex_send.at[n], ex_recv.at[n], partner, m)
        mine = out[pl.ds(pl.multiple_of(64 * k, 64), 64), :]
        wait_bytes(got, ex_recv.at[n])
        return mine + got[...]

    it16 = it.astype(BF16)
    yb[...] = it16
    exchange(yb, rowp, yb, colp, 0)
    wait_some(wp.at[pl.ds(0, 8)], w_recv.at[0], w_kept)
    cross_w(0)
    pending.append(lambda: wait_some(rowp, row_send.at[0], own_row))
    pending.append(lambda: wait_some(colp, col_send.at[0], own_col))
    wait_some(rowp, row_recv.at[0], own_row)
    wait_some(colp, col_recv.at[0], own_col)
    sq = tile_product(rowp, colp, exs, exr, 0)
    pending.append(lambda: wait_bytes(exr, ex_send.at[0]))

    sq16 = sq.astype(BF16)
    ab[...] = sq16
    bb[...] = (0.0625 * sq - 0.5625 * it).astype(BF16)
    exchange(ab, rowp2, bb, colp2, 1)
    cross_w(1)
    pending.append(lambda: wait_bytes(wp.at[pl.ds(0, 8)], w_send.at[1]))
    pending.append(lambda: wait_some(rowp2, row_send.at[1], own_row))
    pending.append(lambda: wait_some(colp2, col_send.at[1], own_col))
    wait_some(rowp2, row_recv.at[1], own_row)
    wait_some(colp2, col_recv.at[1], own_col)
    higher = tile_product(rowp2, colp2, exs2, exr2, 1)
    pending.append(lambda: wait_bytes(exr2, ex_send.at[1]))

    row_ids = m * 128 + 64 * k + lax.broadcasted_iota(jnp.int32, (64, 128), 0)
    col_ids = c * 128 + lax.broadcasted_iota(jnp.int32, (64, 128), 1)
    unit = jnp.where(row_ids == col_ids, 2.25, 0.0).astype(F32)
    zz_tile = unit - 2.4375 * it + 1.6875 * sq + higher
    qb[...] = (higher - 2.4375 * (it - it16.astype(F32)) + 1.6875 * (sq - sq16.astype(F32))).astype(BF16)
    along_row(qb, qp, 2)
    zb[...] = zz_tile
    rcopy(zb, zx, ex_send.at[2], ex_recv.at[2], partner, m)
    pending.append(lambda: wait_some(qp, row_send.at[2], own_row))
    pending.append(lambda: wait_bytes(zx, ex_send.at[2]))

    wait_bytes(zx, ex_recv.at[2])
    whole_tile[pl.ds(pl.multiple_of(64 * k, 64), 64), :] = zb[...]
    whole_tile[pl.ds(pl.multiple_of(64 * (1 - k), 64), 64), :] = zx[...]
    whole_tile[...] = whole_tile[...].T
    root_ref[...] = whole_tile[pl.ds(pl.multiple_of(64 * k, 64), 64), :]

    wait_bytes(wp.at[pl.ds(0, 8)], w_recv.at[1])
    left = 1.6875 * side_by_side(rowp2).astype(F32) - 2.4375 * side_by_side(rowp).astype(F32)
    hi = left.astype(BF16)
    lo = (left - hi.astype(F32)).astype(BF16)

    def weighted(kk, parts):
        cols_kk = jnp.concatenate(
            [wp[8 * (j % 2) + 2 * (j // 2) + kk] for j in range(8)], axis=1)
        return sum(lax.dot_general(cols_kk, p, (((1,), (1,)), ((), ())),
                                   preferred_element_type=F32) for p in parts)

    cxs[...] = weighted(1 - k, (hi, lo))
    cond_ref[...] = weighted(k, (hi, lo)) + 2.25 * wv[...].astype(F32)
    wait_some(qp, row_recv.at[2], own_row)
    rest = side_by_side(qp)
    cxs[...] += weighted(1 - k, (rest,))
    rcopy(cxs, cxr, ex_send.at[3], ex_recv.at[3], partner, m)
    pending.append(lambda: wait_bytes(cxr, ex_send.at[3]))
    cond_ref[...] += weighted(k, (rest,))
    wait_bytes(cxr, ex_recv.at[3])
    cond_ref[...] += cxr[...]

    for finish in pending:
        finish()


def on_device(hidden_grads, weight_grad):
    dma = pltpu.SemaphoreType.DMA
    vm = pltpu.VMEM
    root, conditioned = pl.pallas_call(
        kernel,
        out_shape=(jax.ShapeDtypeStruct((64, 128), F32), jax.ShapeDtypeStruct((192, 128), F32)),
        in_specs=[pl.BlockSpec(memory_space=pltpu.HBM)] * 2,
        out_specs=(pl.BlockSpec(memory_space=pltpu.VMEM),) * 2,
        scratch_shapes=[
            vm((1024, 2048), BF16),
            vm((192, 128), BF16),
            vm((2, 32, 64, 128), BF16),
            vm((64, 64, 128), BF16),
            vm((8, 64, 128), F32), vm((8, 64, 128), F32),
            vm((1, 128), F32), vm((1, 128), F32), vm((1, 128), F32),
            vm((8, 1, 128), F32), vm((1, 128), F32), vm((8, 1, 128), F32),
            vm((64, 128), BF16),
            vm((16, 64, 128), BF16), vm((16, 64, 128), BF16),
            vm((128, 128), F32), vm((64, 128), F32),
            vm((64, 128), BF16), vm((64, 128), BF16),
            vm((16, 64, 128), BF16), vm((16, 64, 128), BF16),
            vm((128, 128), F32), vm((64, 128), F32),
            vm((64, 128), F32), vm((64, 128), F32), vm((128, 128), F32),
            vm((64, 128), BF16), vm((16, 64, 128), BF16),
            vm((16, 192, 128), BF16),
            vm((192, 128), F32), vm((192, 128), F32),
            dma((2,)), dma, dma((3, CH)), dma, dma, dma((2,)), dma((2,)), dma,
            dma, dma, dma((2,)), dma((2,)), dma((3,)), dma((3,)), dma((2,)), dma((2,)), dma((4,)), dma((4,)),
            dma((2,)), dma((2,)), pltpu.SemaphoreType.REGULAR((4,)),
        ],
        compiler_params=pltpu.CompilerParams(has_side_effects=True, collective_id=0, vmem_limit_bytes=56000000),
        name="kfac",
    )(hidden_grads, pltpu.with_memory_space_constraint(weight_grad.T, pltpu.HBM))
    return root.T, conditioned.T


def solution(mesh):
    spec = P("mem", "grp")
    return jax.shard_map(
        on_device,
        mesh=mesh,
        in_specs=(P(("grp", "mem"), None), spec),
        out_specs=(spec, spec),
        check_vma=False,
    )
```

```python
import functools

import jax
import jax.numpy as jnp
from jax import lax
from jax.experimental import pallas as pl
from jax.experimental.pallas import tpu as pltpu
from jax.sharding import PartitionSpec as P

MESH = pl.DeviceIdType.MESH
F32 = jnp.float32
BF16 = jnp.bfloat16
CH = 8
ROWS = 128 // CH
rem = lax.rem
div = lax.div


def rcopy(src, dst, ssem, rsem, g, m):
    cp = pltpu.make_async_remote_copy(
        src_ref=src, dst_ref=dst, send_sem=ssem, recv_sem=rsem,
        device_id=(g, m), device_id_type=MESH,
    )
    cp.start()


FAR_FIRST = (4, 3, 5, 2, 6, 1, 7, 0)


def wait_bytes(ref, sem):
    pltpu.make_async_copy(ref, ref, sem).wait()


def wait_some(ref, sem, fewer):
    @pl.when(fewer)
    def _():
        wait_bytes(ref.at[pl.ds(0, ref.shape[0] - 1)], sem)

    @pl.when(jnp.logical_not(fewer))
    def _():
        wait_bytes(ref, sem)


def kernel(
    x_hbm, w_hbm, root_ref, cond_ref,
    xb, wv, sb, ra, sb2, rb, ss, sso, ssx, ssa, ssy, ssb, yb, rowp, colp, exs, exr,
    ab, bb, rowp2, colp2, exs2, exr2, zb, zx, whole_tile, qb, qp, wp, cxs, cxr,
    lsem, ag_send, ag_recv, fw_send, fw_recv, ss_sem, rs_send, rs_recv, rs2_send, rs2_recv,
    sr_send, sr_recv, row_send, row_recv, col_send, col_recv, ex_send, ex_recv,
    w_send, w_recv, met,
):
    g = lax.axis_index("grp")
    m = lax.axis_index("mem")
    k, c = rem(g, 2), div(g, 2)
    z, xh = div(c, 2), rem(c, 2)
    y, xl = div(m, 2), rem(m, 2)
    x = 2 * xh + xl
    role = rem(x + 2 * y + z, 4)
    partner = c * 2 + 1 - k

    def place(xx, yy, zz, kk):
        return (zz * 2 + div(xx, 2)) * 2 + kk, yy * 2 + rem(xx, 2)

    own = 4 * k
    load_x = pltpu.make_async_copy(x_hbm, xb.at[pl.ds(own * 128, 128)], lsem.at[0])
    load_w = pltpu.make_async_copy(w_hbm, wv, lsem.at[1])
    load_x.start()
    load_w.start()

    barrier = pltpu.get_barrier_semaphore()

    def greet(dg, dm):
        pl.semaphore_signal(barrier, inc=1, device_id=(dg, dm), device_id_type=MESH)

    greet(partner, m)
    for step in (1, 7):
        greet(*place(rem(x + step, 4), y, z, k))
        greet(*place(x, rem(y + step, 8), z, k))
        greet(*place(x, y, rem(z + step, 8), k))
    pl.semaphore_wait(barrier, 7)

    def introduce():
        def nudge(n, dg, dm):
            pl.semaphore_signal(met.at[n], inc=1, device_id=(dg, dm), device_id_type=MESH)

        for step in (1, 3):
            nudge(0, *place(rem(x + step, 4), y, z, k))
        pl.semaphore_wait(met.at[0], 2)
        for n, steps in ((1, (1, 7)), (2, (2, 6))):
            for step in steps:
                nudge(n, *place(x, rem(y + step, 8), z, k))
                nudge(n, *place(x, y, rem(z + step, 8), k))
            pl.semaphore_wait(met.at[n], 4)
        nudge(3, partner, m)
        pl.semaphore_wait(met.at[3], 1)

    def rows(slot, ch):
        return pl.ds(pl.multiple_of(slot * 128 + ch * ROWS, ROWS), ROWS)

    zs_at = [z] + [rem(z + i, 8) for i in range(1, 8)]
    ys_at = [y] + [rem(y + i, 8) for i in range(1, 8)]
    pending = []

    load_x.wait()
    near = (
        place(rem(x + 1 - k, 4), y, rem(z + k, 8), k),
        place(rem(x + 3 * (1 - k), 4), y, rem(z + 7 * k, 8), k),
        place(x, rem(y + 1 + 6 * k, 8), z, k),
    )
    for ch in range(CH):
        for j in range(3):
            rcopy(xb.at[rows(own, ch)], xb.at[rows(own + 1 + j, ch)],
                  ag_send, ag_recv.at[j, ch], *near[j])
    whole = pl.ds(pl.multiple_of(own * 128, 128), 128)
    rcopy(xb.at[whole], xb.at[whole], fw_send, fw_recv, partner, m)
    pending.append(lambda: wait_bytes(xb.at[pl.ds(0, 384)], ag_send))
    pending.append(lambda: wait_bytes(xb.at[pl.ds(0, 512)], fw_send))

    load_w.wait()
    w_slot = 8 * xl + 2 * rem(y, 4) + k
    w_core = div(y, 4)
    w_kept = w_core == k

    def spread_w():
        for i in range(1, 8):
            rcopy(wv, wp.at[w_slot], w_send.at[0], w_recv.at[0], *place(x, ys_at[i], z, w_core))

        @pl.when(w_kept)
        def _():
            wp[w_slot] = wv[...]

        @pl.when(jnp.logical_not(w_kept))
        def _():
            rcopy(wv, wp.at[w_slot], w_send.at[0], w_recv.at[0], partner, m)

    def cross_w(n):
        some = wp.at[pl.ds(8 * xl + 4 * n, 4)]
        rcopy(some, some, w_send.at[1], w_recv.at[1], *place(2 * xh + 1 - xl, y, z, k))

    introduce()
    spread_w()
    pending.append(lambda: wait_some(wp.at[pl.ds(0, 8)], w_send.at[0], w_kept))

    def squares(r):
        v = xb[r, :].astype(F32)
        s = jnp.sum(v * v, axis=0, keepdims=True)
        t = s[:, 0:128]
        for i in range(1, 16):
            t = t + s[:, i * 128:(i + 1) * 128]
        return t

    total = jnp.zeros((1, 128), F32)
    for ch in range(CH):
        total = total + squares(rows(own, ch))
    for ch in range(CH):
        for j in range(3):
            r = rows(own + 1 + j, ch)
            wait_bytes(xb.at[r], ag_recv.at[j, ch])
            rcopy(xb.at[r], xb.at[r], fw_send, fw_recv, partner, m)
        for j in range(3):
            total = total + squares(rows(own + 1 + j, ch))
    ss[...] = total
    rcopy(ss, sso, ss_sem.at[0], ss_sem.at[1], partner, m)
    pending.append(lambda: wait_bytes(ss, ss_sem.at[0]))
    wait_bytes(xb.at[pl.ds(0, 512)], fw_recv)

    def cols(i):
        return xb[:, pl.ds(pl.multiple_of(i * 128, 128), 128)]

    first_slot = z * (1 - k) + y * k
    second_slot = y * (1 - k) + z * k
    in_half = div(y, 4) == k
    on_low = k == 0

    def share_squares():
        wait_bytes(sso, ss_sem.at[1])
        ssx[...] = ss[...] + sso[...]
        ssa[first_slot] = ssx[...]

        for i in FAR_FIRST[:7]:
            yy = (1 - k) * y + k * ys_at[i]
            zz = k * z + (1 - k) * zs_at[i]
            dg, dm = place(rem(role + 24 - 2 * yy - zz, 4), yy, zz, k)
            rcopy(ssx, ssa.at[first_slot], sr_send.at[0], sr_recv.at[0], dg, dm)

    for odd in range(2):
        parity = rem(z + odd, 2)

        @pl.loop(0, 2)
        def _(turn, parity=parity):
            q = parity + 2 * turn
            m0 = 8 * k + rem(role + 4 - q, 4)
            left = jnp.concatenate([cols(m0), cols(m0 + 4)], axis=1)
            zs = [rem(q, 2) + 2 * t for t in range(4)]
            cs = [2 * zt + rem(div(q + 8 - zt, 2), 2) for zt in zs]
            right = jnp.concatenate([cols(ct) for ct in cs], axis=1)
            part = lax.dot_general(left, right, (((0,), (0,)), ((), ())),
                                   preferred_element_type=F32).astype(BF16)
            for a in range(2):
                yo = div(m0 + 4 * a, 2) - 4 * k
                for t in range(4):
                    tile = part[a * 128:(a + 1) * 128, t * 128:(t + 1) * 128]
                    sb[0, zs[t] * 4 + yo] = tile[:64]
                    sb[1, yo * 8 + zs[t]] = tile[64:]

        if odd == 0:
            share_squares()
        for i in FAR_FIRST:
            if i % 2 != odd:
                continue
            zz = zs_at[i]
            piece = sb.at[0, pl.ds(zz * 4, 4)]
            there = pl.ds(z * 8 + 4 * k, 4)
            if i:
                xx = rem(role + 24 - 2 * y - zz, 4)
                rcopy(piece, ra.at[there], rs_send.at[0], rs_recv, *place(xx, y, zz, 0))
                continue

            @pl.when(on_low)
            def _(piece=piece, there=there):
                ra[there] = piece[...]

            @pl.when(jnp.logical_not(on_low))
            def _(piece=piece, there=there):
                rcopy(piece, ra.at[there], rs_send.at[0], rs_recv, partner, m)

    for i in range(1, 5):
        yo = rem(y + i, 4)
        yy = 4 * k + yo
        dg, dm = place(rem(role + 24 - 2 * yy - z, 4), yy, z, 1)
        piece = sb.at[1, pl.ds(yo * 8, 8)]
        there = pl.ds(y * 8, 8)
        mine = jnp.logical_and(k == 1, yy == y)

        @pl.when(mine)
        def _(piece=piece, there=there):
            ra[there] = piece[...]

        @pl.when(jnp.logical_not(mine))
        def _(piece=piece, there=there, dg=dg, dm=dm):
            rcopy(piece, ra.at[there], rs_send.at[1], rs_recv, dg, dm)


    def wait_first(sem, sending):
        full = sb.at[0]
        if sending:
            pl.when(on_low)(lambda: wait_bytes(full.at[pl.ds(0, 28)], sem.at[0]))
            pl.when(k == 1)(lambda: wait_bytes(full, sem.at[0]))
            kept = jnp.logical_and(k == 1, in_half)
            pl.when(kept)(lambda: wait_bytes(full.at[pl.ds(0, 24)], sem.at[1]))
            pl.when(jnp.logical_not(kept))(lambda: wait_bytes(full, sem.at[1]))
        else:
            kept = jnp.logical_and(k == 1, in_half)
            pl.when(on_low)(lambda: wait_bytes(ra.at[pl.ds(0, 60)], sem))
            pl.when(kept)(lambda: wait_bytes(ra.at[pl.ds(0, 56)], sem))
            pl.when(jnp.logical_and(k == 1, jnp.logical_not(in_half)))(lambda: wait_bytes(ra, sem))

    pending.append(lambda: wait_first(rs_send, True))
    pending.append(lambda: wait_bytes(ssa.at[pl.ds(0, 7)], sr_send.at[0]))
    wait_first(rs_recv, False)
    wait_bytes(ssa.at[pl.ds(0, 7)], sr_recv.at[0])
    ssy[...] = jnp.sum(ssa[...], axis=0)

    for i in FAR_FIRST:
        yy = k * y + (1 - k) * ys_at[i]
        zz = (1 - k) * z + k * zs_at[i]
        to = (1 - k) * yy + k * zz
        acc = ra[to].astype(F32)
        for j in range(1, 8):
            acc = acc + ra[j * 8 + to].astype(F32)
        if i:
            dg, dm = place(rem(role + 24 - 2 * yy - zz, 4), yy, zz, k)
            sb2[to] = acc
            rcopy(sb2.at[to], rb.at[second_slot], rs2_send, rs2_recv, dg, dm)
            rcopy(ssy, ssb.at[second_slot], sr_send.at[1], sr_recv.at[1], dg, dm)
        else:
            rb[second_slot] = acc
            ssb[second_slot] = ssy[...]

    pending.append(lambda: wait_bytes(rb.at[pl.ds(0, 7)], rs2_send))
    pending.append(lambda: wait_bytes(ssb.at[pl.ds(0, 7)], sr_send.at[1]))
    wait_bytes(rb.at[pl.ds(0, 7)], rs2_recv)
    wait_bytes(ssb.at[pl.ds(0, 7)], sr_recv.at[1])
    cov = rb[0]
    for j in range(1, 8):
        cov = cov + rb[j]
    total_sq = jnp.sum(ssb[...])
    scale = 2048.0 / (6.0 * total_sq)
    it = cov * scale
    row_core, col_core = div(c, 8), div(m, 8)
    row_slot = 2 * rem(c, 8) + k
    col_slot = 2 * rem(m, 8) + k
    own_row, own_col = row_core == k, col_core == k

    def keep_or_send(mine, src, dst, send, recv, dg, dm):
        @pl.when(mine)
        def _():
            dst[...] = src[...]

        @pl.when(jnp.logical_not(mine))
        def _():
            rcopy(src, dst, send, recv, dg, dm)

    def exchange(row_src, row_dst, col_src, col_dst, n):
        row_to, col_to = row_dst.at[row_slot], col_dst.at[col_slot]
        rs, rr, cs, cr = row_send.at[n], row_recv.at[n], col_send.at[n], col_recv.at[n]
        for i in FAR_FIRST:
            for across in (1, 0):
                xx, ww = (1 - xh, 1 - xl) if across else (xh, xl)
                rg, cg, cm = 4 * zs_at[i] + 2 * xx + row_core, 2 * c + col_core, 2 * ys_at[i] + ww
                if i or across:
                    rcopy(row_src, row_to, rs, rr, rg, m)
                    rcopy(col_src, col_to, cs, cr, cg, cm)
                else:
                    keep_or_send(own_row, row_src, row_to, rs, rr, rg, m)
                    keep_or_send(own_col, col_src, col_to, cs, cr, cg, cm)

    def along_row(src, dst, n):
        to = dst.at[row_slot]
        for zt in range(8):
            dg = 4 * zt + 2 * (1 - xh) + row_core
            rcopy(src, to, row_send.at[n], row_recv.at[n], dg, m)
            dg = 4 * zt + 2 * xh + row_core
            keep_or_send(dg == g, src, to, row_send.at[n], row_recv.at[n], dg, m)

    def side_by_side(ref):
        return jnp.concatenate(
            [ref[2 * j:2 * j + 2].reshape(128, 128) for j in range(8)], axis=1)

    def tile_product(lp, rp, out, got, n):
        out[...] = jnp.dot(side_by_side(lp), rp[...].reshape(1024, 128),
                           preferred_element_type=F32)
        other = pl.ds(pl.multiple_of(64 * (1 - k), 64), 64)
        rcopy(out.at[other], got, ex_send.at[n], ex_recv.at[n], partner, m)
        mine = out[pl.ds(pl.multiple_of(64 * k, 64), 64), :]
        wait_bytes(got, ex_recv.at[n])
        return mine + got[...]

    it16 = it.astype(BF16)
    yb[...] = it16
    exchange(yb, rowp, yb, colp, 0)
    wait_some(wp.at[pl.ds(0, 8)], w_recv.at[0], w_kept)
    cross_w(0)
    pending.append(lambda: wait_some(rowp, row_send.at[0], own_row))
    pending.append(lambda: wait_some(colp, col_send.at[0], own_col))
    wait_some(rowp, row_recv.at[0], own_row)
    wait_some(colp, col_recv.at[0], own_col)
    sq = tile_product(rowp, colp, exs, exr, 0)
    pending.append(lambda: wait_bytes(exr, ex_send.at[0]))

    sq16 = sq.astype(BF16)
    ab[...] = sq16
    bb[...] = (0.0625 * sq - 0.5625 * it).astype(BF16)
    exchange(ab, rowp2, bb, colp2, 1)
    cross_w(1)
    pending.append(lambda: wait_bytes(wp.at[pl.ds(0, 8)], w_send.at[1]))
    pending.append(lambda: wait_some(rowp2, row_send.at[1], own_row))
    pending.append(lambda: wait_some(colp2, col_send.at[1], own_col))
    wait_some(rowp2, row_recv.at[1], own_row)
    wait_some(colp2, col_recv.at[1], own_col)
    higher = tile_product(rowp2, colp2, exs2, exr2, 1)
    pending.append(lambda: wait_bytes(exr2, ex_send.at[1]))

    row_ids = m * 128 + 64 * k + lax.broadcasted_iota(jnp.int32, (64, 128), 0)
    col_ids = c * 128 + lax.broadcasted_iota(jnp.int32, (64, 128), 1)
    unit = jnp.where(row_ids == col_ids, 2.25, 0.0).astype(F32)
    zz_tile = unit - 2.4375 * it + 1.6875 * sq + higher
    qb[...] = (higher - 2.4375 * (it - it16.astype(F32)) + 1.6875 * (sq - sq16.astype(F32))).astype(BF16)
    along_row(qb, qp, 2)
    zb[...] = zz_tile
    rcopy(zb, zx, ex_send.at[2], ex_recv.at[2], partner, m)
    pending.append(lambda: wait_some(qp, row_send.at[2], own_row))
    pending.append(lambda: wait_bytes(zx, ex_send.at[2]))

    wait_bytes(zx, ex_recv.at[2])
    whole_tile[pl.ds(pl.multiple_of(64 * k, 64), 64), :] = zb[...]
    whole_tile[pl.ds(pl.multiple_of(64 * (1 - k), 64), 64), :] = zx[...]
    whole_tile[...] = whole_tile[...].T
    root_ref[...] = whole_tile[pl.ds(pl.multiple_of(64 * k, 64), 64), :]

    wait_bytes(wp.at[pl.ds(0, 8)], w_recv.at[1])
    left = 1.6875 * side_by_side(rowp2).astype(F32) - 2.4375 * side_by_side(rowp).astype(F32)
    hi = left.astype(BF16)
    lo = (left - hi.astype(F32)).astype(BF16)

    def weighted(kk, parts):
        cols_kk = jnp.concatenate(
            [wp[8 * (j % 2) + 2 * (j // 2) + kk] for j in range(8)], axis=1)
        return sum(lax.dot_general(cols_kk, p, (((1,), (1,)), ((), ())),
                                   preferred_element_type=F32) for p in parts)

    cxs[...] = weighted(1 - k, (hi, lo))
    cond_ref[...] = weighted(k, (hi, lo)) + 2.25 * wv[...].astype(F32)
    wait_some(qp, row_recv.at[2], own_row)
    rest = side_by_side(qp)
    cxs[...] += weighted(1 - k, (rest,))
    rcopy(cxs, cxr, ex_send.at[3], ex_recv.at[3], partner, m)
    pending.append(lambda: wait_bytes(cxr, ex_send.at[3]))
    cond_ref[...] += weighted(k, (rest,))
    wait_bytes(cxr, ex_recv.at[3])
    cond_ref[...] += cxr[...]

    for finish in pending:
        finish()


def on_device(hidden_grads, weight_grad):
    dma = pltpu.SemaphoreType.DMA
    vm = pltpu.VMEM
    root, conditioned = pl.pallas_call(
        kernel,
        out_shape=(jax.ShapeDtypeStruct((64, 128), F32), jax.ShapeDtypeStruct((192, 128), F32)),
        in_specs=[pl.BlockSpec(memory_space=pltpu.HBM)] * 2,
        out_specs=(pl.BlockSpec(memory_space=pltpu.VMEM),) * 2,
        scratch_shapes=[
            vm((1024, 2048), BF16),
            vm((192, 128), BF16),
            vm((2, 32, 64, 128), BF16),
            vm((64, 64, 128), BF16),
            vm((8, 64, 128), F32), vm((8, 64, 128), F32),
            vm((1, 128), F32), vm((1, 128), F32), vm((1, 128), F32),
            vm((8, 1, 128), F32), vm((1, 128), F32), vm((8, 1, 128), F32),
            vm((64, 128), BF16),
            vm((16, 64, 128), BF16), vm((16, 64, 128), BF16),
            vm((128, 128), F32), vm((64, 128), F32),
            vm((64, 128), BF16), vm((64, 128), BF16),
            vm((16, 64, 128), BF16), vm((16, 64, 128), BF16),
            vm((128, 128), F32), vm((64, 128), F32),
            vm((64, 128), F32), vm((64, 128), F32), vm((128, 128), F32),
            vm((64, 128), BF16), vm((16, 64, 128), BF16),
            vm((16, 192, 128), BF16),
            vm((192, 128), F32), vm((192, 128), F32),
            dma((2,)), dma, dma((3, CH)), dma, dma, dma((2,)), dma((2,)), dma,
            dma, dma, dma((2,)), dma((2,)), dma((3,)), dma((3,)), dma((2,)), dma((2,)), dma((4,)), dma((4,)),
            dma((2,)), dma((2,)), pltpu.SemaphoreType.REGULAR((4,)),
        ],
        compiler_params=pltpu.CompilerParams(has_side_effects=True, collective_id=0, vmem_limit_bytes=56000000),
        name="kfac",
    )(hidden_grads, pltpu.with_memory_space_constraint(weight_grad.T, pltpu.HBM))
    return root.T, conditioned.T


def solution(mesh):
    spec = P("mem", "grp")
    return jax.shard_map(
        on_device,
        mesh=mesh,
        in_specs=(P(("grp", "mem"), None), spec),
        out_specs=(spec, spec),
        check_vma=False,
    )
```
